16 devices in a mesh: stage: 2 (over z), expert: 8 (over y, x, core).
Axes of the slice: x: 2, y: 2, z: 2, core: 2. Of those that a mesh axis runs over, the one named last changes fastest.
Arguments:
- tokens_in: bfloat16 [2, 2048, 768], P('stage', 'expert')
- expert_ids: int32 [2, 2048, 1], P('stage', 'expert')
- gate_wts: float32 [2, 2048, 1], P('stage', 'expert')
- w_gate: bfloat16 [2, 8, 768, 3072], P('stage', 'expert')
- w_up: bfloat16 [2, 8, 768, 3072], P('stage', 'expert')
- w_down: bfloat16 [2, 8, 3072, 768], P('stage', 'expert')
- grad_out: bfloat16 [2, 2048, 768], P('stage', 'expert')
Outputs:
- output 1: bfloat16 [2, 2048, 768], P('stage', 'expert')
- output 2: bfloat16 [2, 2048, 768], P('stage', 'expert')
- output 3: bfloat16 [2, 8, 768, 3072], P('stage', 'expert')
- output 4: bfloat16 [2, 8, 768, 3072], P('stage', 'expert')
- output 5: bfloat16 [2, 8, 3072, 768], P('stage', 'expert')
All inputs are finite; a program needn't handle non-finite values.
Results may differ from the reference program's by a relative error of at most 0.001.
Values are sent between devices in bfloat16 or wider.
A program may use at most 1 GiB of HBM per device.

```python
import jax
import jax.numpy as jnp
from jax import lax

STAGE_SIZE = 2
GROUP_SIZE = 8
TOKENS_DEV = 256
D_MODEL = 768
D_FF = 3072
EXPERTS = 8
TOP_K = 1

HALF_STAGE = STAGE_SIZE // 2
LANE_TOKENS = GROUP_SIZE * TOKENS_DEV
CAPACITY = 3 * TOKENS_DEV * TOP_K // (2 * EXPERTS)


def route_source(src_key):
    key_perm, key_pair, key_tok = jax.random.split(src_key, 3)
    base_count = TOKENS_DEV * TOP_K // EXPERTS
    half_count = base_count // 2
    run_order = jax.random.permutation(key_perm, EXPERTS)
    pair_shift = jax.random.randint(key_pair, (EXPERTS // 2,), 0, half_count + 1)
    pair_shift = pair_shift.at[0].set(half_count)
    counts = jnp.stack([base_count + pair_shift, base_count - pair_shift], axis=1).reshape(EXPERTS)
    run_ends = jnp.cumsum(counts)
    tok_perm = jax.random.permutation(key_tok, TOKENS_DEV)
    flat_pos = tok_perm[:, None] + TOKENS_DEV * jnp.arange(TOP_K)[None, :]
    run_ids = jnp.searchsorted(run_ends, flat_pos, side="right")
    return run_order[run_ids].astype(jnp.int32)


def setup_inputs(seed: int = 0) -> dict:
    key_list = jax.random.split(jax.random.key(seed), 7)
    tok_shape = (STAGE_SIZE, LANE_TOKENS, D_MODEL)
    tokens_in = jax.random.normal(key_list[0], tok_shape, jnp.float32)
    src_keys = jax.random.split(key_list[1], STAGE_SIZE * GROUP_SIZE)
    expert_ids = jax.vmap(route_source)(src_keys).reshape(STAGE_SIZE, LANE_TOKENS, TOP_K)
    gate_wts = jax.random.uniform(key_list[2], (STAGE_SIZE, LANE_TOKENS, TOP_K), jnp.float32, 0.5, 1.5) * TOP_K ** -0.5
    w_gate = jax.random.normal(key_list[3], (STAGE_SIZE, EXPERTS, D_MODEL, D_FF), jnp.float32) * D_MODEL ** -0.5
    w_up = jax.random.normal(key_list[4], (STAGE_SIZE, EXPERTS, D_MODEL, D_FF), jnp.float32) * D_MODEL ** -0.5
    w_down = jax.random.normal(key_list[5], (STAGE_SIZE, EXPERTS, D_FF, D_MODEL), jnp.float32) * D_FF ** -0.5
    grad_out = jax.random.normal(key_list[6], tok_shape, jnp.float32)
    return {
        "tokens_in": tokens_in.astype(jnp.bfloat16),
        "expert_ids": expert_ids,
        "gate_wts": gate_wts,
        "w_gate": w_gate.astype(jnp.bfloat16),
        "w_up": w_up.astype(jnp.bfloat16),
        "w_down": w_down.astype(jnp.bfloat16),
        "grad_out": grad_out.astype(jnp.bfloat16),
    }


def lane_pass(lane_in):
    tokens, expert_ids, gate_wts, w_gate, w_up, w_down, grad_out = lane_in
    asg_count = LANE_TOKENS * TOP_K
    buf_rows = GROUP_SIZE * CAPACITY
    flat_ids = expert_ids.reshape(asg_count)
    tok_pad = jnp.concatenate([tokens, jnp.zeros((1, D_MODEL), tokens.dtype)], axis=0)
    dy_pad = jnp.concatenate([grad_out, jnp.zeros((1, D_MODEL), grad_out.dtype)], axis=0)
    gate_pad = jnp.concatenate([gate_wts.reshape(asg_count), jnp.zeros((1,), jnp.float32)])

    def expert_step(carry, expert_in):
        y_acc, dx_acc = carry
        expert_num, w_gate_e, w_up_e, w_down_e = expert_in
        is_hit = (flat_ids == expert_num).astype(jnp.int32)
        buf_pos = jnp.where(is_hit > 0, jnp.cumsum(is_hit) - 1, buf_rows)
        asg_row = jnp.full((buf_rows,), asg_count, jnp.int32).at[buf_pos].set(jnp.arange(asg_count, dtype=jnp.int32), mode="drop")
        tok_row = asg_row // TOP_K
        x_rows = tok_pad[tok_row]
        gate_row = gate_pad[asg_row]
        pre_gate = jnp.dot(x_rows, w_gate_e, preferred_element_type=jnp.float32)
        pre_up = jnp.dot(x_rows, w_up_e, preferred_element_type=jnp.float32)
        sig_gate = jax.nn.sigmoid(pre_gate)
        act_gate = pre_gate * sig_gate
        hidden = (act_gate * pre_up).astype(jnp.bfloat16)
        out_rows = jnp.dot(hidden, w_down_e, preferred_element_type=jnp.float32).astype(jnp.bfloat16)
        y_acc = y_acc + jax.ops.segment_sum(gate_row[:, None] * out_rows.astype(jnp.float32), tok_row, num_segments=LANE_TOKENS + 1)
        g_out = (gate_row[:, None] * dy_pad[tok_row].astype(jnp.float32)).astype(jnp.bfloat16)
        d_hidden = jnp.dot(g_out, w_down_e.T, preferred_element_type=jnp.float32)
        d_gate = (d_hidden * pre_up * sig_gate * (1.0 + pre_gate * (1.0 - sig_gate))).astype(jnp.bfloat16)
        d_up = (d_hidden * act_gate).astype(jnp.bfloat16)
        dx_rows = (jnp.dot(d_gate, w_gate_e.T, preferred_element_type=jnp.float32) + jnp.dot(d_up, w_up_e.T, preferred_element_type=jnp.float32)).astype(jnp.bfloat16)
        dx_acc = dx_acc + jax.ops.segment_sum(dx_rows.astype(jnp.float32), tok_row, num_segments=LANE_TOKENS + 1)
        grad_wg = jnp.dot(x_rows.T, d_gate, preferred_element_type=jnp.float32).astype(jnp.bfloat16)
        grad_wu = jnp.dot(x_rows.T, d_up, preferred_element_type=jnp.float32).astype(jnp.bfloat16)
        grad_wd = jnp.dot(hidden.T, g_out, preferred_element_type=jnp.float32).astype(jnp.bfloat16)
        return (y_acc, dx_acc), (grad_wg, grad_wu, grad_wd)

    zero_acc = jnp.zeros((LANE_TOKENS + 1, D_MODEL), jnp.float32)
    expert_in = (jnp.arange(EXPERTS, dtype=jnp.int32), w_gate, w_up, w_down)
    (y_acc, dx_acc), (grad_wg, grad_wu, grad_wd) = lax.scan(expert_step, (zero_acc, zero_acc), expert_in)
    return y_acc[:LANE_TOKENS].astype(jnp.bfloat16), dx_acc[:LANE_TOKENS].astype(jnp.bfloat16), grad_wg, grad_wu, grad_wd


def reference(tokens_in, expert_ids, gate_wts, w_gate, w_up, w_down, grad_out):
    lane_in = (
        tokens_in[:HALF_STAGE],
        expert_ids[:HALF_STAGE],
        gate_wts[:HALF_STAGE],
        w_gate[HALF_STAGE:],
        w_up[HALF_STAGE:],
        w_down[HALF_STAGE:],
        grad_out[HALF_STAGE:],
    )
    y_b, dx_a, grad_wg, grad_wu, grad_wd = lax.map(lane_pass, lane_in)
    y_out = jnp.concatenate([jnp.zeros_like(y_b), y_b], axis=0)
    grad_tokens = jnp.concatenate([dx_a, jnp.zeros_like(dx_a)], axis=0)
    grad_w_gate = jnp.concatenate([jnp.zeros_like(grad_wg), grad_wg], axis=0)
    grad_w_up = jnp.concatenate([jnp.zeros_like(grad_wu), grad_wu], axis=0)
    grad_w_down = jnp.concatenate([jnp.zeros_like(grad_wd), grad_wd], axis=0)
    return (y_out, grad_tokens, grad_w_gate, grad_w_up, grad_w_down)
```

```python
import functools

import jax
import jax.numpy as jnp
from jax import lax
from jax.experimental import pallas as pl
from jax.experimental.pallas import tpu as pltpu
from jax.sharding import PartitionSpec as P

MESH = pl.DeviceIdType.MESH
BF16 = jnp.bfloat16
F32 = jnp.float32
COL = 256
TILE = 256
NT = (((1,), (1,)), ((), ()))
TN = (((0,), (0,)), ((), ()))


def dot(lhs, rhs, dims=(((1,), (0,)), ((), ()))):
    return lax.dot_general(lhs, rhs, dims, preferred_element_type=F32)


def slot_matrix(ids_row, n_exp, cap):
    n_tok = ids_row.shape[1]
    held = lax.broadcasted_iota(jnp.int32, (n_exp, n_tok), 0) == ids_row
    earlier = lax.broadcasted_iota(jnp.int32, (n_tok, n_tok), 0) < lax.broadcasted_iota(jnp.int32, (n_tok, n_tok), 1)
    counts = dot(held.astype(BF16), earlier.astype(BF16))
    rank = jnp.sum(jnp.where(held, counts, 0.0), axis=0, keepdims=True)
    slot = ids_row * cap + rank.astype(jnp.int32)
    return (lax.broadcasted_iota(jnp.int32, (n_exp * cap, n_tok), 0) == slot).astype(BF16)


def gate_column(gate_row):
    n_tok = gate_row.shape[1]
    eye = lax.broadcasted_iota(jnp.int32, (n_tok, n_tok), 0) == lax.broadcasted_iota(jnp.int32, (n_tok, n_tok), 1)
    return jnp.sum(jnp.where(eye, gate_row, 0.0), axis=1, keepdims=True)


def exchange_kernel(
    n_group, cap,
    ids_ref, gate_ref, x_ref, dy_ref, w1_hbm, w3_hbm, w2_hbm,
    y_ref, dx_ref, xr, qr, h_ref, da_ref, db_ref,
    w1, w3, w2, a_acc, b_acc, dh_acc, perm, xs, qs, dxs, dxr, os, yr, ids_m, gate_m,
    w_sem, meta_sem, xsend, xrecv, qsend, qrecv, dxsend, dxrecv, osend, yrecv,
):
    stage = lax.axis_index("stage")
    me = lax.axis_index("expert")
    n_chunk = xs.shape[0]
    n_rows = n_group * cap
    d_ff = w1.shape[1]
    n_tile = d_ff // TILE
    on_a = stage == 0
    on_b = stage == 1

    def block(index):
        return pl.ds(pl.multiple_of(index * cap, 16), cap)

    def send(src, dst, send_sem, recv_sem, to_stage, to):
        pltpu.make_async_remote_copy(
            src_ref=src, dst_ref=dst, send_sem=send_sem, recv_sem=recv_sem,
            device_id=(to_stage, to), device_id_type=MESH,
        ).start()

    def wait_recv(ref, sem):
        pltpu.make_async_copy(ref, ref, sem).wait()

    barrier = pltpu.get_barrier_semaphore()
    for other in range(1, 2 * n_group):
        flat = lax.rem(stage * n_group + me + other, 2 * n_group)
        pl.semaphore_signal(
            barrier, inc=1, device_id=(flat // n_group, lax.rem(flat, n_group)), device_id_type=MESH
        )

    w2_copy = pltpu.make_async_copy(w2_hbm, w2, w_sem.at[0])
    w1_copies = []
    w3_copies = []
    for c in range(n_chunk):
        rows = pl.ds(c * COL, COL)
        w1_copies.append(pltpu.make_async_copy(w1_hbm.at[rows], w1.at[rows], w_sem.at[1 + 2 * c]))
        w3_copies.append(pltpu.make_async_copy(w3_hbm.at[rows], w3.at[rows], w_sem.at[2 + 2 * c]))

    @pl.when(on_b)
    def _():
        w2_copy.start()
        for c in range(n_chunk):
            w1_copies[c].start()
            w3_copies[c].start()

    @pl.when(on_a)
    def _():
        perm[...] = slot_matrix(ids_ref[...], n_group, cap)
        xs[0] = dot(perm[...], x_ref[:, :COL]).astype(BF16)

    pl.semaphore_wait(barrier, 2 * n_group - 1)

    @pl.when(on_a)
    def _():
        send(ids_ref, ids_m, meta_sem.at[0], meta_sem.at[2], 1, me)
        send(gate_ref, gate_m, meta_sem.at[1], meta_sem.at[3], 1, me)
        for c in range(n_chunk):
            if c > 0:
                xs[c] = dot(perm[...], x_ref[:, c * COL:(c + 1) * COL]).astype(BF16)
            for k in range(n_group):
                to = lax.rem(me + k, n_group)
                send(xs.at[c, block(to)], xr.at[c, block(me)], xsend, xrecv.at[c], 1, to)
        y_ref[...] = jnp.zeros_like(y_ref)
        for c in range(n_chunk):
            wait_recv(dxr.at[c], dxrecv.at[c])
            dx_ref[:, c * COL:(c + 1) * COL] = dot(perm[...], dxr[c], TN).astype(BF16)
        wait_recv(ids_ref, meta_sem.at[0])
        wait_recv(gate_ref, meta_sem.at[1])
        wait_recv(xs, xsend)

    @pl.when(on_b)
    def _():
        wait_recv(ids_m, meta_sem.at[2])
        wait_recv(gate_m, meta_sem.at[3])
        perm[...] = slot_matrix(ids_m[...], n_group, cap)
        gate_col = gate_column(gate_m[...])
        gated = (gate_col * dy_ref[...].astype(F32)).astype(BF16)
        qs[...] = dot(perm[...], gated).astype(BF16)
        for k in range(1, n_group):
            to = lax.rem(me + k, n_group)
            send(qs.at[block(to)], qr.at[block(me)], qsend, qrecv, 1, to)
        qr[block(me), :] = qs[block(me), :]
        dx_ref[...] = jnp.zeros_like(dx_ref)
        w2_copy.wait()
        others = pl.ds(0, n_rows - cap)
        wait_recv(qr.at[others], qrecv)

        @pl.loop(0, n_tile)
        def _(j):
            cols = pl.ds(pl.multiple_of(j * TILE, TILE), TILE)
            dh_acc[:, cols] = dot(qr[...], w2[cols, :], NT)

        for c in range(n_chunk):
            w1_copies[c].wait()
            w3_copies[c].wait()
            wait_recv(xr.at[c], xrecv.at[c])
            rows = slice(c * COL, (c + 1) * COL)

            @pl.loop(0, n_tile)
            def _(j):
                cols = pl.ds(pl.multiple_of(j * TILE, TILE), TILE)
                a = dot(xr[c], w1[rows, cols])
                b = dot(xr[c], w3[rows, cols])
                if c > 0:
                    a = a + a_acc[:, cols]
                    b = b + b_acc[:, cols]
                if c < n_chunk - 1:
                    a_acc[:, cols] = a
                    b_acc[:, cols] = b
                else:
                    dh = dh_acc[:, cols]
                    sig = jax.nn.sigmoid(a)
                    act = a * sig
                    h_ref[:, cols] = (act * b).astype(BF16)
                    da_ref[:, cols] = (dh * b * sig * (1.0 + a * (1.0 - sig))).astype(BF16)
                    db_ref[:, cols] = (dh * act).astype(BF16)

        for c in range(n_chunk):
            rows = slice(c * COL, (c + 1) * COL)
            dxs[c] = (dot(da_ref[...], w1[rows, :], NT) + dot(db_ref[...], w3[rows, :], NT)).astype(BF16)
            for k in range(n_group):
                to = lax.rem(me + k, n_group)
                send(dxs.at[c, block(to)], dxr.at[c, block(me)], dxsend, dxrecv.at[c], 0, to)
        for c in range(n_chunk):
            os[c] = dot(h_ref[...], w2[:, c * COL:(c + 1) * COL]).astype(BF16)
            for k in range(1, n_group):
                to = lax.rem(me + k, n_group)
                send(os.at[c, block(to)], yr.at[c, block(me)], osend, yrecv.at[c], 1, to)
            yr[c, block(me), :] = os[c, block(me), :]
        for c in range(n_chunk):
            wait_recv(yr.at[c, others], yrecv.at[c])
            y_ref[:, c * COL:(c + 1) * COL] = (gate_col * dot(perm[...], yr[c], TN)).astype(BF16)
        wait_recv(qs.at[others], qsend)
        wait_recv(dxs, dxsend)
        wait_recv(os.at[:, others], osend)


def weight_grad_kernel(xr, qr, h_ref, da_ref, db_ref, y_in, dx_in, dw1, dw3, dw2, y_ref, dx_ref):
    step = pl.program_id(0)
    stage = lax.axis_index("stage")
    n_chunk = xr.shape[0]
    cols = pl.ds(pl.multiple_of(step * TILE, TILE), TILE)

    @pl.when(step == 0)
    def _():
        y_ref[...] = y_in[...]
        dx_ref[...] = dx_in[...]

    @pl.when(stage == 1)
    def _():
        for c in range(n_chunk):
            rows = slice(c * COL, (c + 1) * COL)
            dw1[rows, :] = dot(xr[c], da_ref[:, cols], TN).astype(BF16)
            dw3[rows, :] = dot(xr[c], db_ref[:, cols], TN).astype(BF16)
        dw2[...] = dot(h_ref[:, cols], qr[...], TN).astype(BF16)

    @pl.when(stage == 0)
    def _():
        dw1[...] = jnp.zeros_like(dw1)
        dw3[...] = jnp.zeros_like(dw3)
        dw2[...] = jnp.zeros_like(dw2)


def solution(mesh):
    n_group = mesh.shape["expert"]
    tok_spec = P("stage", "expert", None)
    w_spec = P("stage", "expert", None, None)

    def device_fn(tokens_in, expert_ids, gate_wts, w_gate, w_up, w_down, grad_out):
        n_tok, d_model = tokens_in.shape[1:]
        d_ff = w_gate.shape[3]
        cap = 3 * n_tok // (2 * n_group)
        n_rows = n_group * cap
        n_chunk = d_model // COL
        vmem = pl.BlockSpec(memory_space=pltpu.VMEM)
        hbm = pl.BlockSpec(memory_space=pl.ANY)
        chunked = (n_chunk, n_rows, COL)
        dma = pltpu.SemaphoreType.DMA
        y, dx, xr, qr, h, da, db = pl.pallas_call(
            functools.partial(exchange_kernel, n_group, cap),
            out_shape=(
                pltpu.VMEM((n_tok, d_model), BF16),
                pltpu.VMEM((n_tok, d_model), BF16),
                pltpu.VMEM(chunked, BF16),
                pltpu.VMEM((n_rows, d_model), BF16),
                pltpu.VMEM((n_rows, d_ff), BF16),
                pltpu.VMEM((n_rows, d_ff), BF16),
                pltpu.VMEM((n_rows, d_ff), BF16),
            ),
            in_specs=[vmem] * 4 + [hbm] * 3,
            out_specs=(vmem,) * 7,
            scratch_shapes=[
                pltpu.VMEM((d_model, d_ff), BF16),
                pltpu.VMEM((d_model, d_ff), BF16),
                pltpu.VMEM((d_ff, d_model), BF16),
                pltpu.VMEM((n_rows, d_ff), F32),
                pltpu.VMEM((n_rows, d_ff), F32),
                pltpu.VMEM((n_rows, d_ff), F32),
                pltpu.VMEM((n_rows, n_tok), BF16),
                pltpu.VMEM(chunked, BF16),
                pltpu.VMEM((n_rows, d_model), BF16),
                pltpu.VMEM(chunked, BF16),
                pltpu.VMEM(chunked, BF16),
                pltpu.VMEM(chunked, BF16),
                pltpu.VMEM(chunked, BF16),
                pltpu.VMEM((1, n_tok), jnp.int32),
                pltpu.VMEM((1, n_tok), F32),
                dma((1 + 2 * n_chunk,)),
                dma((4,)),
                dma(()),
                dma((n_chunk,)),
                dma(()),
                dma(()),
                dma(()),
                dma((n_chunk,)),
                dma(()),
                dma((n_chunk,)),
            ],
            compiler_params=pltpu.CompilerParams(
                collective_id=0, has_side_effects=True, vmem_limit_bytes=48 * 2**20
            ),
            name="exchange",
        )(
            expert_ids.reshape(1, n_tok), gate_wts.reshape(1, n_tok), tokens_in[0], grad_out[0],
            w_gate[0, 0], w_up[0, 0], w_down[0, 0],
        )
        held = [pltpu.with_memory_space_constraint(v, pltpu.VMEM) for v in (xr, qr, h, da, db, y, dx)]
        whole = pl.BlockSpec((n_tok, d_model), lambda j: (0, 0))
        dw1, dw3, dw2, y, dx = pl.pallas_call(
            weight_grad_kernel,
            grid=(d_ff // TILE,),
            out_shape=(
                jax.ShapeDtypeStruct((d_model, d_ff), BF16),
                jax.ShapeDtypeStruct((d_model, d_ff), BF16),
                jax.ShapeDtypeStruct((d_ff, d_model), BF16),
                jax.ShapeDtypeStruct((n_tok, d_model), BF16),
                jax.ShapeDtypeStruct((n_tok, d_model), BF16),
            ),
            in_specs=[vmem] * 7,
            out_specs=(
                pl.BlockSpec((d_model, TILE), lambda j: (0, j)),
                pl.BlockSpec((d_model, TILE), lambda j: (0, j)),
                pl.BlockSpec((TILE, d_model), lambda j: (j, 0)),
                whole,
                whole,
            ),
            compiler_params=pltpu.CompilerParams(vmem_limit_bytes=24 * 2**20),
            name="weight_grad",
        )(*held)
        return y[None], dx[None], dw1[None, None], dw3[None, None], dw2[None, None]

    return jax.shard_map(
        device_fn,
        mesh=mesh,
        in_specs=(tok_spec, tok_spec, tok_spec, w_spec, w_spec, w_spec, tok_spec),
        out_specs=(tok_spec, tok_spec, w_spec, w_spec, w_spec),
        check_vma=False,
    )
```

```python
import functools

import jax
import jax.numpy as jnp
from jax import lax
from jax.experimental import pallas as pl
from jax.experimental.pallas import tpu as pltpu
from jax.sharding import PartitionSpec as P

MESH = pl.DeviceIdType.MESH
BF16 = jnp.bfloat16
F32 = jnp.float32
COL = 256
TILE = 256
N_CHUNK = 2
NT = (((1,), (1,)), ((), ()))
TN = (((0,), (0,)), ((), ()))
PEERS = ((0, 0, 0), (0, 0, 1), (1, 1, 0), (1, 1, 1), (0, 1, 0), (0, 1, 1), (1, 0, 0), (1, 0, 1))


def dot(lhs, rhs, dims=(((1,), (0,)), ((), ()))):
    return lax.dot_general(lhs, rhs, dims, preferred_element_type=F32)


def peer(me, place):
    y, x, core = PEERS[place]
    flip_y = lax.rem(me // 4 + y, 2)
    flip_x = lax.rem(lax.rem(me // 2, 2) + x, 2)
    return flip_y * 4 + flip_x * 2 + lax.rem(lax.rem(me, 2) + core, 2)


def slot_matrix(ids_row, n_exp, cap):
    n_tok = ids_row.shape[1]
    held = lax.broadcasted_iota(jnp.int32, (n_exp, n_tok), 0) == ids_row
    earlier = lax.broadcasted_iota(jnp.int32, (n_tok, n_tok), 0) < lax.broadcasted_iota(jnp.int32, (n_tok, n_tok), 1)
    counts = dot(held.astype(BF16), earlier.astype(BF16))
    rank = jnp.sum(jnp.where(held, counts, 0.0), axis=0, keepdims=True)
    slot = ids_row * cap + rank.astype(jnp.int32)
    return (lax.broadcasted_iota(jnp.int32, (n_exp * cap, n_tok), 0) == slot).astype(BF16)


def gate_column(gate_row):
    n_tok = gate_row.shape[1]
    eye = lax.broadcasted_iota(jnp.int32, (n_tok, n_tok), 0) == lax.broadcasted_iota(jnp.int32, (n_tok, n_tok), 1)
    return jnp.sum(jnp.where(eye, gate_row, 0.0), axis=1, keepdims=True)


def exchange_kernel(
    n_group, cap,
    ids_ref, gate_ref, x_ref, dy_ref, w1_hbm, w3_hbm, w2_hbm,
    y_ref, dx_ref, xt, db_ref, dw1, dw2,
    w1, w3, w2, xr, qr, h_ref, da_ref, perm, xs, qs, dxs, dxr, os, yr, ids_m, gate_m,
    w_sem, meta_sem, xsend, xrecv, qsend, qrecv, dxsend, dxrecv, osend, yrecv,
):
    stage = lax.axis_index("stage")
    me = lax.axis_index("expert")
    n_rows = n_group * cap
    d_model, d_ff = w1.shape
    n_col = d_model // COL
    per = n_group // N_CHUNK
    on_a = stage == 0
    on_b = stage == 1

    def block(index):
        return pl.ds(pl.multiple_of(index * cap, 16), cap)

    def place(k):
        return pl.ds(k * cap, cap)

    def send(src, dst, send_sem, recv_sem, to_stage, to):
        pltpu.make_async_remote_copy(
            src_ref=src, dst_ref=dst, send_sem=send_sem, recv_sem=recv_sem,
            device_id=(to_stage, to), device_id_type=MESH,
        ).start()

    def wait_bytes(ref, sem):
        pltpu.make_async_copy(ref, ref, sem).wait()

    barrier = pltpu.get_barrier_semaphore()
    for other in range(1, 2 * n_group):
        flat = lax.rem(stage * n_group + me + other, 2 * n_group)
        pl.semaphore_signal(
            barrier, inc=1, device_id=(flat // n_group, lax.rem(flat, n_group)), device_id_type=MESH
        )
    loads = [pltpu.make_async_copy(src, dst, w_sem.at[i]) for i, (src, dst) in enumerate(((w2_hbm, w2), (w1_hbm, w1), (w3_hbm, w3)))]

    @pl.when(on_b)
    def _():
        for load in loads:
            load.start()

    @pl.when(on_a)
    def _():
        perm[...] = slot_matrix(ids_ref[...], n_group, cap)
        xs[...] = dot(perm[...], x_ref[...]).astype(BF16)

    pl.semaphore_wait(barrier, 2 * n_group - 1)

    @pl.when(on_a)
    def _():
        send(ids_ref, ids_m, meta_sem.at[0], meta_sem.at[2], 1, me)
        send(gate_ref, gate_m, meta_sem.at[1], meta_sem.at[3], 1, me)
        for k in range(n_group):
            to = peer(me, k)
            send(xs.at[block(to)], xr.at[place(k)], xsend, xrecv.at[k // per], 1, to)
        y_ref[...] = jnp.zeros_like(y_ref)
        dw1[...] = jnp.zeros_like(dw1)
        dw2[...] = jnp.zeros_like(dw2)
        for c in range(n_col):
            wait_bytes(dxr.at[c], dxrecv.at[c])
            dx_ref[:, c * COL:(c + 1) * COL] = dot(perm[...], dxr[c], TN).astype(BF16)
        wait_bytes(ids_ref, meta_sem.at[0])
        wait_bytes(gate_ref, meta_sem.at[1])
        wait_bytes(xs, xsend)

    @pl.when(on_b)
    def _():
        wait_bytes(ids_m, meta_sem.at[2])
        wait_bytes(gate_m, meta_sem.at[3])
        perm[...] = slot_matrix(ids_m[...], n_group, cap)
        gate_col = gate_column(gate_m[...])
        gated = (gate_col * dy_ref[...].astype(F32)).astype(BF16)
        qs[...] = dot(perm[...], gated).astype(BF16)
        for k in range(1, n_group):
            to = peer(me, k)
            send(qs.at[block(to)], qr.at[place(k)], qsend, qrecv.at[k // per], 1, to)
        qr[place(0), :] = qs[block(me), :]
        dx_ref[...] = jnp.zeros_like(dx_ref)
        for load in loads:
            load.wait()
        for r in range(N_CHUNK):
            first = 1 if r == 0 else r * per
            wait_bytes(qr.at[pl.ds(first * cap, ((r + 1) * per - first) * cap)], qrecv.at[r])
            rows = slice(r * per * cap, (r + 1) * per * cap)
            wait_bytes(xr.at[pl.ds(r * per * cap, per * cap)], xrecv.at[r])
            for j in range(d_ff // TILE):
                cols = slice(j * TILE, (j + 1) * TILE)
                dh = dot(qr[rows, :], w2[cols, :], NT)
                a = dot(xr[rows, :], w1[:, cols])
                b = dot(xr[rows, :], w3[:, cols])
                sig = jax.nn.sigmoid(a)
                act = a * sig
                h_ref[rows, cols] = (act * b).astype(BF16)
                da_ref[rows, cols] = (dh * b * sig * (1.0 + a * (1.0 - sig))).astype(BF16)
                db_ref[rows, cols] = (dh * act).astype(BF16)
            for c in range(n_col):
                cols = slice(c * COL, (c + 1) * COL)
                dxs[c, rows, :] = (dot(da_ref[rows, :], w1[cols, :], NT) + dot(db_ref[rows, :], w3[cols, :], NT)).astype(BF16)
                for k in range(r * per, (r + 1) * per):
                    send(dxs.at[c, place(k)], dxr.at[c, block(me)], dxsend, dxrecv.at[c], 0, peer(me, k))
            os[rows, :] = dot(h_ref[rows, :], w2[...]).astype(BF16)
            for k in range(r * per, (r + 1) * per):
                if k > 0:
                    send(os.at[place(k)], yr.at[block(me)], osend, yrecv, 1, peer(me, k))
            if r == 0:
                yr[block(me), :] = os[place(0), :]
        for j in range(d_ff // TILE):
            cols = slice(j * TILE, (j + 1) * TILE)
            dw2[cols, :] = dot(h_ref[:, cols], qr[...], TN).astype(BF16)
        xt[...] = xr[...].T
        for j in range(d_ff // TILE):
            cols = slice(j * TILE, (j + 1) * TILE)
            dw1[:, cols] = dot(xt[...], da_ref[:, cols]).astype(BF16)
        others = pl.ds(0, n_rows - cap)
        wait_bytes(yr.at[others], yrecv)
        y_ref[...] = (gate_col * dot(perm[...], yr[...], TN)).astype(BF16)
        wait_bytes(qs.at[others], qsend)
        wait_bytes(dxs, dxsend)
        wait_bytes(os.at[others], osend)


def store_kernel(xt, db_ref, dw1_in, dw2_in, y_in, dx_in, dw1, dw3, dw2, y_out, dx_out, dw3_v, sem, sem3):
    stage = lax.axis_index("stage")
    d_ff = db_ref.shape[1]
    pairs = ((dw2_in, dw2), (dw1_in, dw1), (y_in, y_out), (dx_in, dx_out))
    copies = [pltpu.make_async_copy(src, dst, sem.at[i]) for i, (src, dst) in enumerate(pairs)]
    for copy in copies:
        copy.start()

    @pl.when(stage == 0)
    def _():
        copy = pltpu.make_async_copy(dw1_in, dw3, sem3.at[0])
        copy.start()
        copy.wait()

    @pl.when(stage == 1)
    def _():
        pieces = []
        for j in range(d_ff // (2 * TILE)):
            cols = pl.ds(j * 2 * TILE, 2 * TILE)
            dw3_v[:, cols] = dot(xt[...], db_ref[:, cols]).astype(BF16)
            pieces.append(pltpu.make_async_copy(dw3_v.at[:, cols], dw3.at[:, cols], sem3.at[j]))
            pieces[-1].start()
        for piece in pieces:
            piece.wait()

    for copy in copies:
        copy.wait()


def solution(mesh):
    n_group = mesh.shape["expert"]
    tok_spec = P("stage", "expert", None)
    w_spec = P("stage", "expert", None, None)

    def device_fn(tokens_in, expert_ids, gate_wts, w_gate, w_up, w_down, grad_out):
        n_tok, d_model = tokens_in.shape[1:]
        d_ff = w_gate.shape[3]
        cap = 3 * n_tok // (2 * n_group)
        n_rows = n_group * cap
        vmem = pl.BlockSpec(memory_space=pltpu.VMEM)
        hbm = pl.BlockSpec(memory_space=pl.ANY)
        blocks = pltpu.VMEM((n_rows, d_model), BF16)
        pieces = pltpu.VMEM((d_model // COL, n_rows, COL), BF16)
        hidden = pltpu.VMEM((n_rows, d_ff), BF16)
        up = pltpu.VMEM((d_model, d_ff), BF16)
        down = pltpu.VMEM((d_ff, d_model), BF16)
        tok = pltpu.VMEM((n_tok, d_model), BF16)
        dma = pltpu.SemaphoreType.DMA
        y, dx, xt, db, dw1, dw2 = pl.pallas_call(
            functools.partial(exchange_kernel, n_group, cap),
            out_shape=(tok, tok, pltpu.VMEM((d_model, n_rows), BF16), hidden, up, down),
            in_specs=[vmem] * 4 + [hbm] * 3,
            out_specs=(vmem,) * 6,
            scratch_shapes=[
                up, up, down, blocks, blocks, hidden, hidden,
                pltpu.VMEM((n_rows, n_tok), BF16),
                blocks, blocks, pieces, pieces, blocks, blocks,
                pltpu.VMEM((1, n_tok), jnp.int32),
                pltpu.VMEM((1, n_tok), F32),
                dma((3,)),
                dma((4,)),
                dma(()),
                dma((N_CHUNK,)),
                dma(()),
                dma((N_CHUNK,)),
                dma(()),
                dma((d_model // COL,)),
                dma(()),
                dma(()),
            ],
            compiler_params=pltpu.CompilerParams(
                collective_id=0, has_side_effects=True, vmem_limit_bytes=40 * 2**20
            ),
            name="exchange",
        )(
            expert_ids.reshape(1, n_tok), gate_wts.reshape(1, n_tok), tokens_in[0], grad_out[0],
            w_gate[0, 0], w_up[0, 0], w_down[0, 0],
        )
        held = [pltpu.with_memory_space_constraint(v, pltpu.VMEM) for v in (xt, db, dw1, dw2, y, dx)]
        dw1, dw3, dw2, y, dx = pl.pallas_call(
            store_kernel,
            out_shape=(
                jax.ShapeDtypeStruct((d_model, d_ff), BF16),
                jax.ShapeDtypeStruct((d_model, d_ff), BF16),
                jax.ShapeDtypeStruct((d_ff, d_model), BF16),
                jax.ShapeDtypeStruct((n_tok, d_model), BF16),
                jax.ShapeDtypeStruct((n_tok, d_model), BF16),
            ),
            in_specs=[vmem] * 6,
            out_specs=(hbm,) * 5,
            scratch_shapes=[up, dma((4,)), dma((d_ff // (2 * TILE),))],
            compiler_params=pltpu.CompilerParams(vmem_limit_bytes=16 * 2**20),
            name="store",
        )(*held)
        return y[None], dx[None], dw1[None, None], dw3[None, None], dw2[None, None]

    return jax.shard_map(
        device_fn,
        mesh=mesh,
        in_specs=(tok_spec, tok_spec, tok_spec, w_spec, w_spec, w_spec, tok_spec),
        out_specs=(tok_spec, tok_spec, w_spec, w_spec, w_spec),
        check_vma=False,
    )
```

```python
import functools

import jax
import jax.numpy as jnp
from jax import lax
from jax.experimental import pallas as pl
from jax.experimental.pallas import tpu as pltpu
from jax.sharding import PartitionSpec as P

MESH = pl.DeviceIdType.MESH
BF16 = jnp.bfloat16
F32 = jnp.float32
COL = 256
TILE = 256
N_CHUNK = 2
WIDE = 768
WINDOW = 1
NT = (((1,), (1,)), ((), ()))
TN = (((0,), (0,)), ((), ()))
PEERS = ((0, 0, 0), (0, 0, 1), (1, 1, 0), (1, 1, 1), (0, 1, 0), (0, 1, 1), (1, 0, 0), (1, 0, 1))


def dot(lhs, rhs, dims=(((1,), (0,)), ((), ()))):
    return lax.dot_general(lhs, rhs, dims, preferred_element_type=F32)


def peer(me, place):
    y, x, core = PEERS[place]
    flip_y = lax.rem(me // 4 + y, 2)
    flip_x = lax.rem(lax.rem(me // 2, 2) + x, 2)
    return flip_y * 4 + flip_x * 2 + lax.rem(lax.rem(me, 2) + core, 2)


def slot_matrix(ids_row, n_exp, cap):
    n_tok = ids_row.shape[1]
    held = lax.broadcasted_iota(jnp.int32, (n_exp, n_tok), 0) == ids_row
    earlier = lax.broadcasted_iota(jnp.int32, (n_tok, n_tok), 0) < lax.broadcasted_iota(jnp.int32, (n_tok, n_tok), 1)
    counts = dot(held.astype(BF16), earlier.astype(BF16))
    rank = jnp.sum(jnp.where(held, counts, 0.0), axis=0, keepdims=True)
    slot = ids_row * cap + rank.astype(jnp.int32)
    return (lax.broadcasted_iota(jnp.int32, (n_exp * cap, n_tok), 0) == slot).astype(BF16)


def gate_column(gate_row):
    n_tok = gate_row.shape[1]
    eye = lax.broadcasted_iota(jnp.int32, (n_tok, n_tok), 0) == lax.broadcasted_iota(jnp.int32, (n_tok, n_tok), 1)
    return jnp.sum(jnp.where(eye, gate_row, 0.0), axis=1, keepdims=True)


def exchange_kernel(
    n_group, cap,
    ids_hbm, gate_hbm, x_hbm, dy_hbm, w1_hbm, w3_hbm, w2_hbm,
    y_ref, dx_ref, xt, db_ref, dw1, dw2,
    w1, w3, w2, xr, qr, h_ref, da_ref, perm, xs, qs, dxs, dxr, os, yr, ids_m, gate_m, tok_v,
    w_sem, in_sem, meta_sem, xsend, xrecv, qsend, qrecv, dxsend, dxrecv, osend, yrecv,
):
    stage = lax.axis_index("stage")
    me = lax.axis_index("expert")
    n_rows = n_group * cap
    d_model, d_ff = w1.shape
    n_col = d_model // COL
    per = n_group // N_CHUNK
    on_a = stage == 0
    on_b = stage == 1

    def block(index):
        return pl.ds(pl.multiple_of(index * cap, 16), cap)

    def place(k):
        return pl.ds(k * cap, cap)

    def send(src, dst, send_sem, recv_sem, to_stage, to):
        pltpu.make_async_remote_copy(
            src_ref=src, dst_ref=dst, send_sem=send_sem, recv_sem=recv_sem,
            device_id=(to_stage, to), device_id_type=MESH,
        ).start()

    def wait_bytes(ref, sem):
        pltpu.make_async_copy(ref, ref, sem).wait()

    barrier = pltpu.get_barrier_semaphore()
    for other in range(1, 2 * n_group):
        flat = lax.rem(stage * n_group + me + other, 2 * n_group)
        pl.semaphore_signal(
            barrier, inc=1, device_id=(flat // n_group, lax.rem(flat, n_group)), device_id_type=MESH
        )
    loads = [pltpu.make_async_copy(src, dst, w_sem.at[i]) for i, (src, dst) in enumerate(((w2_hbm, w2), (w1_hbm, w1), (w3_hbm, w3)))]

    ids_load = pltpu.make_async_copy(ids_hbm, ids_m, in_sem.at[0])
    gate_load = pltpu.make_async_copy(gate_hbm, gate_m, in_sem.at[1])
    x_load = pltpu.make_async_copy(x_hbm, tok_v, in_sem.at[2])
    dy_load = pltpu.make_async_copy(dy_hbm, tok_v, in_sem.at[2])

    @pl.when(on_b)
    def _():
        dy_load.start()
        for load in loads:
            load.start()

    @pl.when(on_a)
    def _():
        ids_load.start()
        gate_load.start()
        x_load.start()
        ids_load.wait()
        gate_load.wait()
        perm[...] = slot_matrix(ids_m[...], n_group, cap)
        x_load.wait()
        xs[...] = dot(perm[...], tok_v[...]).astype(BF16)

    pl.semaphore_wait(barrier, 2 * n_group - 1)

    @pl.when(on_a)
    def _():
        send(ids_m, ids_m, meta_sem.at[0], meta_sem.at[2], 1, me)
        send(gate_m, gate_m, meta_sem.at[1], meta_sem.at[3], 1, me)
        for k in range(n_group):
            to = peer(me, k)
            if k >= WINDOW:
                wait_bytes(xs.at[place(0)], xsend.at[k - WINDOW])
            send(xs.at[block(to)], xr.at[place(k)], xsend.at[k], xrecv.at[k // per], 1, to)
        for k in range(n_group - WINDOW, n_group):
            wait_bytes(xs.at[place(0)], xsend.at[k])
        y_ref[...] = jnp.zeros_like(y_ref)

        @pl.loop(0, d_ff // WIDE)
        def _(j):
            cols = pl.ds(pl.multiple_of(j * WIDE, WIDE), WIDE)
            dw1[:, cols] = jnp.zeros((d_model, WIDE), BF16)
            dw2[cols, :] = jnp.zeros((WIDE, d_model), BF16)

        for c in range(n_col):
            wait_bytes(dxr.at[c], dxrecv.at[c])
            dx_ref[:, c * COL:(c + 1) * COL] = dot(perm[...], dxr[c], TN).astype(BF16)
        wait_bytes(ids_m, meta_sem.at[0])
        wait_bytes(gate_m, meta_sem.at[1])

    @pl.when(on_b)
    def _():
        wait_bytes(ids_m, meta_sem.at[2])
        wait_bytes(gate_m, meta_sem.at[3])
        perm[...] = slot_matrix(ids_m[...], n_group, cap)
        gate_col = gate_column(gate_m[...])
        dy_load.wait()
        gated = (gate_col * tok_v[...].astype(F32)).astype(BF16)
        qs[...] = dot(perm[...], gated).astype(BF16)
        for r in range(N_CHUNK):
            for k in range(max(1, r * per), (r + 1) * per):
                to = peer(me, k)
                send(qs.at[block(to)], qr.at[place(k)], qsend.at[r], qrecv.at[r], 1, to)
            if r == 0:
                qr[place(0), :] = qs[block(me), :]
                dx_ref[...] = jnp.zeros_like(dx_ref)
                wait_bytes(qs.at[pl.ds(0, (per - 1) * cap)], qsend.at[r])
        for load in loads:
            load.wait()
        for r in range(N_CHUNK):
            first = 1 if r == 0 else r * per
            wait_bytes(qr.at[pl.ds(first * cap, ((r + 1) * per - first) * cap)], qrecv.at[r])
            rows = slice(r * per * cap, (r + 1) * per * cap)
            wait_bytes(xr.at[pl.ds(r * per * cap, per * cap)], xrecv.at[r])
            for j in range(d_ff // TILE):
                cols = slice(j * TILE, (j + 1) * TILE)
                dh = dot(qr[rows, :], w2[cols, :], NT)
                a = dot(xr[rows, :], w1[:, cols])
                b = dot(xr[rows, :], w3[:, cols])
                sig = jax.nn.sigmoid(a)
                act = a * sig
                h_ref[rows, cols] = (act * b).astype(BF16)
                da_ref[rows, cols] = (dh * b * sig * (1.0 + a * (1.0 - sig))).astype(BF16)
                db_ref[rows, cols] = (dh * act).astype(BF16)

            @pl.loop(0, n_col)
            def _(c):
                cols = pl.ds(pl.multiple_of(c * COL, COL), COL)
                dxs[c, rows, :] = (dot(da_ref[rows, :], w1[cols, :], NT) + dot(db_ref[rows, :], w3[cols, :], NT)).astype(BF16)
                for k in range(r * per, (r + 1) * per):
                    send(dxs.at[c, place(k)], dxr.at[c, block(me)], dxsend, dxrecv.at[c], 0, peer(me, k))

            @pl.loop(0, n_col)
            def _(c):
                cols = pl.ds(pl.multiple_of(c * COL, COL), COL)
                os[rows, cols] = dot(h_ref[rows, :], w2[:, cols]).astype(BF16)

            for k in range(r * per, (r + 1) * per):
                if k > 0:
                    send(os.at[place(k)], yr.at[block(me)], osend, yrecv, 1, peer(me, k))
            if r == 0:
                yr[block(me), :] = os[place(0), :]
        @pl.loop(0, d_ff // WIDE)
        def _(j):
            cols = pl.ds(pl.multiple_of(j * WIDE, WIDE), WIDE)
            dw2[cols, :] = dot(h_ref[:, cols], qr[...], TN).astype(BF16)
        xt[...] = xr[...].T

        @pl.loop(0, d_ff // WIDE)
        def _(j):
            cols = pl.ds(pl.multiple_of(j * WIDE, WIDE), WIDE)
            dw1[:, cols] = dot(xt[...], da_ref[:, cols]).astype(BF16)

        others = pl.ds(0, n_rows - cap)
        wait_bytes(yr.at[others], yrecv)
        y_ref[...] = (gate_col * dot(perm[...], yr[...], TN)).astype(BF16)
        wait_bytes(qs.at[pl.ds(0, per * cap)], qsend.at[1])
        wait_bytes(dxs, dxsend)
        wait_bytes(os.at[others], osend)


def store_kernel(xt, db_ref, dw1_in, dw2_in, y_in, dx_in, dw1, dw3, dw2, y_out, dx_out, dw3_v, sem, sem3):
    stage = lax.axis_index("stage")
    d_ff = db_ref.shape[1]
    pairs = ((dw2_in, dw2), (dw1_in, dw1), (y_in, y_out), (dx_in, dx_out))
    copies = [pltpu.make_async_copy(src, dst, sem.at[i]) for i, (src, dst) in enumerate(pairs)]
    for copy in copies:
        copy.start()

    @pl.when(stage == 0)
    def _():
        copy = pltpu.make_async_copy(dw1_in, dw3, sem3.at[0])
        copy.start()
        copy.wait()

    @pl.when(stage == 1)
    def _():
        pieces = []
        for j in range(d_ff // (2 * TILE)):
            cols = pl.ds(j * 2 * TILE, 2 * TILE)
            dw3_v[:, cols] = dot(xt[...], db_ref[:, cols]).astype(BF16)
            pieces.append(pltpu.make_async_copy(dw3_v.at[:, cols], dw3.at[:, cols], sem3.at[j]))
            pieces[-1].start()
        for piece in pieces:
            piece.wait()

    for copy in copies:
        copy.wait()


def solution(mesh):
    n_group = mesh.shape["expert"]
    tok_spec = P("stage", "expert", None)
    w_spec = P("stage", "expert", None, None)

    def device_fn(tokens_in, expert_ids, gate_wts, w_gate, w_up, w_down, grad_out):
        n_tok, d_model = tokens_in.shape[1:]
        d_ff = w_gate.shape[3]
        cap = 3 * n_tok // (2 * n_group)
        n_rows = n_group * cap
        vmem = pl.BlockSpec(memory_space=pltpu.VMEM)
        hbm = pl.BlockSpec(memory_space=pl.ANY)
        blocks = pltpu.VMEM((n_rows, d_model), BF16)
        pieces = pltpu.VMEM((d_model // COL, n_rows, COL), BF16)
        hidden = pltpu.VMEM((n_rows, d_ff), BF16)
        up = pltpu.VMEM((d_model, d_ff), BF16)
        down = pltpu.VMEM((d_ff, d_model), BF16)
        tok = pltpu.VMEM((n_tok, d_model), BF16)
        dma = pltpu.SemaphoreType.DMA
        y, dx, xt, db, dw1, dw2 = pl.pallas_call(
            functools.partial(exchange_kernel, n_group, cap),
            out_shape=(tok, tok, pltpu.VMEM((d_model, n_rows), BF16), hidden, up, down),
            in_specs=[hbm] * 7,
            out_specs=(vmem,) * 6,
            scratch_shapes=[
                up, up, down, blocks, blocks, hidden, hidden,
                pltpu.VMEM((n_rows, n_tok), BF16),
                blocks, blocks, pieces, pieces, blocks, blocks,
                pltpu.VMEM((1, n_tok), jnp.int32),
                pltpu.VMEM((1, n_tok), F32),
                tok,
                dma((3,)),
                dma((3,)),
                dma((4,)),
                dma((n_group,)),
                dma((N_CHUNK,)),
                dma((N_CHUNK,)),
                dma((N_CHUNK,)),
                dma(()),
                dma((d_model // COL,)),
                dma(()),
                dma(()),
            ],
            compiler_params=pltpu.CompilerParams(
                collective_id=0, has_side_effects=True, vmem_limit_bytes=40 * 2**20
            ),
            name="exchange",
        )(*(pltpu.with_memory_space_constraint(v, pltpu.HBM) for v in (
            expert_ids.reshape(1, n_tok), gate_wts.reshape(1, n_tok), tokens_in[0], grad_out[0],
            w_gate[0, 0], w_up[0, 0], w_down[0, 0],
        )))
        held = [pltpu.with_memory_space_constraint(v, pltpu.VMEM) for v in (xt, db, dw1, dw2, y, dx)]
        dw1, dw3, dw2, y, dx = pl.pallas_call(
            store_kernel,
            out_shape=(
                jax.ShapeDtypeStruct((d_model, d_ff), BF16),
                jax.ShapeDtypeStruct((d_model, d_ff), BF16),
                jax.ShapeDtypeStruct((d_ff, d_model), BF16),
                jax.ShapeDtypeStruct((n_tok, d_model), BF16),
                jax.ShapeDtypeStruct((n_tok, d_model), BF16),
            ),
            in_specs=[vmem] * 6,
            out_specs=(hbm,) * 5,
            scratch_shapes=[up, dma((4,)), dma((d_ff // (2 * TILE),))],
            compiler_params=pltpu.CompilerParams(vmem_limit_bytes=16 * 2**20),
            name="store",
        )(*held)
        return y[None], dx[None], dw1[None, None], dw3[None, None], dw2[None, None]

    return jax.shard_map(
        device_fn,
        mesh=mesh,
        in_specs=(tok_spec, tok_spec, tok_spec, w_spec, w_spec, w_spec, tok_spec),
        out_specs=(tok_spec, tok_spec, w_spec, w_spec, w_spec),
        check_vma=False,
    )
```

```python
import functools

import jax
import jax.numpy as jnp
from jax import lax
from jax.experimental import pallas as pl
from jax.experimental.pallas import tpu as pltpu
from jax.sharding import PartitionSpec as P

MESH = pl.DeviceIdType.MESH
BF16 = jnp.bfloat16
F32 = jnp.float32
COL = 256
PIECE = 512
TILE = 256
CHUNKS = ((0, 4), (4, 8))
HERE = 1536
WIDE = 768
THIRD = 16
WINDOWS = (9, 4)
NT = (((1,), (1,)), ((), ()))
TN = (((0,), (0,)), ((), ()))
PEERS = ((0, 0, 0), (0, 0, 1), (1, 1, 0), (1, 1, 1), (0, 1, 0), (0, 1, 1), (1, 0, 0), (1, 0, 1))


def dot(lhs, rhs, dims=(((1,), (0,)), ((), ()))):
    return lax.dot_general(lhs, rhs, dims, preferred_element_type=F32)


def peer(me, place):
    y, x, core = PEERS[place]
    flip_y = lax.rem(me // 4 + y, 2)
    flip_x = lax.rem(lax.rem(me // 2, 2) + x, 2)
    return flip_y * 4 + flip_x * 2 + lax.rem(lax.rem(me, 2) + core, 2)


def slot_matrix(ids_row, n_exp, cap):
    n_tok = ids_row.shape[1]
    held = lax.broadcasted_iota(jnp.int32, (n_exp, n_tok), 0) == ids_row
    earlier = lax.broadcasted_iota(jnp.int32, (n_tok, n_tok), 0) < lax.broadcasted_iota(jnp.int32, (n_tok, n_tok), 1)
    counts = dot(held.astype(BF16), earlier.astype(BF16))
    rank = jnp.sum(jnp.where(held, counts, 0.0), axis=0, keepdims=True)
    slot = ids_row * cap + rank.astype(jnp.int32)
    return (lax.broadcasted_iota(jnp.int32, (n_exp * cap, n_tok), 0) == slot).astype(BF16)


def gate_column(gate_row):
    n_tok = gate_row.shape[1]
    eye = lax.broadcasted_iota(jnp.int32, (n_tok, n_tok), 0) == lax.broadcasted_iota(jnp.int32, (n_tok, n_tok), 1)
    return jnp.sum(jnp.where(eye, gate_row, 0.0), axis=1, keepdims=True)


def exchange_kernel(
    n_group, cap,
    ids_hbm, gate_hbm, x_hbm, dy_hbm, w1_hbm, w3_hbm, w2_hbm,
    y_ref, dx_ref, xt, da_ref, db_ref, dw1, dw2,
    w1, w3, w2, w1t, w3t, w2t, xr, qr, h_ref, perm, xs, qs, dxs, dxr, os, yr, ids_m, gate_m, tok_v,
    w_sem, in_sem, meta_sem, xsend, xrecv, qsend, qrecv, dxsend, dxrecv, osend, yrecv,
):
    stage = lax.axis_index("stage")
    me = lax.axis_index("expert")
    n_rows = n_group * cap
    d_model, d_ff = w1.shape
    n_col = d_model // COL
    chunk_of = [r for r, (lo, hi) in enumerate(CHUNKS) for _ in range(lo, hi)]
    on_a = stage == 0
    on_b = stage == 1

    def block(index):
        return pl.ds(pl.multiple_of(index * cap, 16), cap)

    def place(k):
        return pl.ds(k * cap, cap)

    def send(src, dst, send_sem, recv_sem, to_stage, to):
        pltpu.make_async_remote_copy(
            src_ref=src, dst_ref=dst, send_sem=send_sem, recv_sem=recv_sem,
            device_id=(to_stage, to), device_id_type=MESH,
        ).start()

    def wait_bytes(ref, sem):
        pltpu.make_async_copy(ref, ref, sem).wait()

    barrier = pltpu.get_barrier_semaphore()
    for other in range(1, 2 * n_group):
        flat = lax.rem(stage * n_group + me + other, 2 * n_group)
        pl.semaphore_signal(
            barrier, inc=1, device_id=(flat // n_group, lax.rem(flat, n_group)), device_id_type=MESH
        )
    loads = [pltpu.make_async_copy(src, dst, w_sem.at[i]) for i, (src, dst) in enumerate(((w2_hbm, w2), (w1_hbm, w1), (w3_hbm, w3)))]

    ids_load = pltpu.make_async_copy(ids_hbm, ids_m, in_sem.at[0])
    gate_load = pltpu.make_async_copy(gate_hbm, gate_m, in_sem.at[1])
    x_load = pltpu.make_async_copy(x_hbm, tok_v, in_sem.at[2])
    dy_load = pltpu.make_async_copy(dy_hbm, tok_v, in_sem.at[2])

    @pl.when(on_b)
    def _():
        dy_load.start()
        for load in loads:
            load.start()

    @pl.when(on_a)
    def _():
        ids_load.start()
        gate_load.start()
        x_load.start()
        ids_load.wait()
        gate_load.wait()
        perm[...] = slot_matrix(ids_m[...], n_group, cap)
        x_load.wait()
        xs[...] = dot(perm[...], tok_v[...]).astype(BF16)

    pl.semaphore_wait(barrier, 2 * n_group - 1)

    @pl.when(on_a)
    def _():
        send(ids_m, ids_m, meta_sem.at[0], meta_sem.at[2], 1, me)
        send(gate_m, gate_m, meta_sem.at[1], meta_sem.at[3], 1, me)
        n_third = cap // THIRD

        def send_x(window):
            for p in range(n_group * n_third):
                k, part = divmod(p, n_third)
                to = peer(me, k)
                if p >= window:
                    wait_bytes(xs.at[pl.ds(0, THIRD)], xsend.at[p % window])
                src = pl.ds(pl.multiple_of(to * cap + part * THIRD, THIRD), THIRD)
                dst = pl.ds(k * cap + part * THIRD, THIRD)
                send(xs.at[src], xr.at[dst], xsend.at[p % window], xrecv.at[chunk_of[k]], 1, to)
            for p in range(window):
                wait_bytes(xs.at[pl.ds(0, THIRD)], xsend.at[p])

        for core, window in enumerate(WINDOWS):
            pl.when(lax.rem(me, 2) == core)(functools.partial(send_x, window))
        y_ref[...] = jnp.zeros_like(y_ref)

        @pl.loop(0, d_ff // WIDE)
        def _(j):
            cols = pl.ds(pl.multiple_of(j * WIDE, WIDE), WIDE)
            dw2[cols, :] = jnp.zeros((WIDE, d_model), BF16)

        @pl.loop(0, HERE // WIDE)
        def _(j):
            cols = pl.ds(pl.multiple_of(j * WIDE, WIDE), WIDE)
            dw1[:, cols] = jnp.zeros((d_model, WIDE), BF16)

        for c in range(n_col):
            wait_bytes(dxr.at[c], dxrecv.at[c])
            dx_ref[:, c * COL:(c + 1) * COL] = dot(perm[...], dxr[c], TN).astype(BF16)
        wait_bytes(ids_m, meta_sem.at[0])
        wait_bytes(gate_m, meta_sem.at[1])

    @pl.when(on_b)
    def _():
        eye = (
            lax.broadcasted_iota(jnp.int32, (TILE, TILE), 0) == lax.broadcasted_iota(jnp.int32, (TILE, TILE), 1)
        ).astype(BF16)
        loads[0].wait()

        @pl.loop(0, d_ff // WIDE)
        def _(j):
            for c in range(n_col):
                wide = pl.ds(pl.multiple_of(j * WIDE, WIDE), WIDE)
                cols = slice(c * COL, (c + 1) * COL)
                w2t[cols, wide] = dot(eye, w2[wide, cols], NT).astype(BF16)

        wait_bytes(ids_m, meta_sem.at[2])
        wait_bytes(gate_m, meta_sem.at[3])
        perm[...] = slot_matrix(ids_m[...], n_group, cap)
        gate_col = gate_column(gate_m[...])
        dy_load.wait()
        gated = (gate_col * tok_v[...].astype(F32)).astype(BF16)
        qs[...] = dot(perm[...], gated).astype(BF16)

        def send_q(r):
            for k in range(max(1, CHUNKS[r][0]), CHUNKS[r][1]):
                to = peer(me, k)
                send(qs.at[block(to)], qr.at[place(k)], qsend, qrecv.at[r], 1, to)

        send_q(0)
        for load, src, dst in ((loads[1], w1, w1t), (loads[2], w3, w3t)):
            load.wait()

            @pl.loop(0, d_ff // WIDE)
            def _(j):
                for i in range(WIDE // TILE):
                    tile = pl.ds(pl.multiple_of(j * WIDE + i * TILE, TILE), TILE)
                    dst[tile, :] = dot(eye, src[:, tile], NT).astype(BF16)

        send_q(1)
        qr[place(0), :] = qs[block(me), :]
        dx_ref[...] = jnp.zeros_like(dx_ref)
        for r, (lo, hi) in enumerate(CHUNKS):
            first = max(1, lo)
            wait_bytes(qr.at[pl.ds(first * cap, (hi - first) * cap)], qrecv.at[r])
            rows = slice(lo * cap, hi * cap)
            wait_bytes(xr.at[pl.ds(lo * cap, (hi - lo) * cap)], xrecv.at[r])
            for j in range(d_ff // TILE):
                cols = slice(j * TILE, (j + 1) * TILE)
                dh = dot(qr[rows, :], w2t[:, cols])
                a = dot(xr[rows, :], w1[:, cols])
                b = dot(xr[rows, :], w3[:, cols])
                sig = jax.nn.sigmoid(a)
                act = a * sig
                h_ref[rows, cols] = (act * b).astype(BF16)
                da_ref[rows, cols] = (dh * b * sig * (1.0 + a * (1.0 - sig))).astype(BF16)
                db_ref[rows, cols] = (dh * act).astype(BF16)

            @pl.loop(0, n_col)
            def _(c):
                cols = pl.ds(pl.multiple_of(c * COL, COL), COL)
                dxs[c, rows, :] = (dot(da_ref[rows, :], w1t[:, cols]) + dot(db_ref[rows, :], w3t[:, cols])).astype(BF16)
                for k in range(lo, hi):
                    send(dxs.at[c, place(k)], dxr.at[c, block(me)], dxsend, dxrecv.at[c], 0, peer(me, k))

            @pl.loop(0, n_col)
            def _(c):
                cols = pl.ds(pl.multiple_of(c * COL, COL), COL)
                os[rows, cols] = dot(h_ref[rows, :], w2[:, cols]).astype(BF16)

            for k in range(lo, hi):
                if k > 0:
                    send(os.at[place(k)], yr.at[block(me)], osend, yrecv, 1, peer(me, k))
            if r == 0:
                yr[block(me), :] = os[place(0), :]
        @pl.loop(0, d_ff // WIDE)
        def _(j):
            cols = pl.ds(pl.multiple_of(j * WIDE, WIDE), WIDE)
            dw2[cols, :] = dot(h_ref[:, cols], qr[...], TN).astype(BF16)
        xt[...] = xr[...].T

        @pl.loop(0, HERE // WIDE)
        def _(j):
            cols = pl.ds(pl.multiple_of(j * WIDE, WIDE), WIDE)
            dw1[:, cols] = dot(xt[...], da_ref[:, cols]).astype(BF16)

        others = pl.ds(0, n_rows - cap)
        wait_bytes(yr.at[others], yrecv)
        y_ref[...] = (gate_col * dot(perm[...], yr[...], TN)).astype(BF16)
        wait_bytes(qs.at[others], qsend)
        wait_bytes(dxs, dxsend)
        wait_bytes(os.at[others], osend)


def store_kernel(xt, da_ref, db_ref, dw1_in, dw2_in, y_in, dx_in, dw1, dw3, dw2, y_out, dx_out, dw1_v, dw3_v, sem, piece_sem):
    stage = lax.axis_index("stage")
    d_ff = db_ref.shape[1]
    pairs = ((dw2_in, dw2), (dw1_in, dw1.at[:, pl.ds(0, HERE)]), (y_in, y_out), (dx_in, dx_out))
    copies = [pltpu.make_async_copy(src, dst, sem.at[i]) for i, (src, dst) in enumerate(pairs)]
    for copy in copies:
        copy.start()

    @pl.when(stage == 0)
    def _():
        places = [dw1.at[:, pl.ds(HERE, d_ff - HERE)], dw3.at[:, pl.ds(0, HERE)], dw3.at[:, pl.ds(HERE, d_ff - HERE)]]
        zeros = [pltpu.make_async_copy(dw1_in.at[:, pl.ds(0, dst.shape[1])], dst, piece_sem.at[i]) for i, dst in enumerate(places)]
        for copy in zeros:
            copy.start()
        for copy in zeros:
            copy.wait()

    @pl.when(stage == 1)
    def _():
        pieces = []
        for grad, held, out, skip in ((da_ref, dw1_v, dw1, HERE), (db_ref, dw3_v, dw3, 0)):
            for j in range((d_ff - skip) // PIECE):
                here = pl.ds(j * PIECE, PIECE)
                there = pl.ds(skip + j * PIECE, PIECE)
                held[:, here] = dot(xt[...], grad[:, there]).astype(BF16)
                pieces.append(pltpu.make_async_copy(held.at[:, here], out.at[:, there], piece_sem.at[len(pieces)]))
                pieces[-1].start()
        for piece in pieces:
            piece.wait()

    for copy in copies:
        copy.wait()


def solution(mesh):
    n_group = mesh.shape["expert"]
    tok_spec = P("stage", "expert", None)
    w_spec = P("stage", "expert", None, None)

    def device_fn(tokens_in, expert_ids, gate_wts, w_gate, w_up, w_down, grad_out):
        n_tok, d_model = tokens_in.shape[1:]
        d_ff = w_gate.shape[3]
        cap = 3 * n_tok // (2 * n_group)
        n_rows = n_group * cap
        vmem = pl.BlockSpec(memory_space=pltpu.VMEM)
        hbm = pl.BlockSpec(memory_space=pl.ANY)
        blocks = pltpu.VMEM((n_rows, d_model), BF16)
        pieces = pltpu.VMEM((d_model // COL, n_rows, COL), BF16)
        hidden = pltpu.VMEM((n_rows, d_ff), BF16)
        up = pltpu.VMEM((d_model, d_ff), BF16)
        down = pltpu.VMEM((d_ff, d_model), BF16)
        tok = pltpu.VMEM((n_tok, d_model), BF16)
        dma = pltpu.SemaphoreType.DMA
        y, dx, xt, da, db, dw1, dw2 = pl.pallas_call(
            functools.partial(exchange_kernel, n_group, cap),
            out_shape=(tok, tok, pltpu.VMEM((d_model, n_rows), BF16), hidden, hidden, pltpu.VMEM((d_model, HERE), BF16), down),
            in_specs=[hbm] * 7,
            out_specs=(vmem,) * 7,
            scratch_shapes=[
                up, up, down, down, down, up, blocks, blocks, hidden,
                pltpu.VMEM((n_rows, n_tok), BF16),
                blocks, blocks, pieces, pieces, blocks, blocks,
                pltpu.VMEM((1, n_tok), jnp.int32),
                pltpu.VMEM((1, n_tok), F32),
                tok,
                dma((3,)),
                dma((3,)),
                dma((4,)),
                dma((max(WINDOWS),)),
                dma((len(CHUNKS),)),
                dma(()),
                dma((len(CHUNKS),)),
                dma(()),
                dma((d_model // COL,)),
                dma(()),
                dma(()),
            ],
            compiler_params=pltpu.CompilerParams(
                collective_id=0, has_side_effects=True, vmem_limit_bytes=48 * 2**20
            ),
            name="exchange",
        )(*(pltpu.with_memory_space_constraint(v, pltpu.HBM) for v in (
            expert_ids.reshape(1, n_tok), gate_wts.reshape(1, n_tok), tokens_in[0], grad_out[0],
            w_gate[0, 0], w_up[0, 0], w_down[0, 0],
        )))
        held = [pltpu.with_memory_space_constraint(v, pltpu.VMEM) for v in (xt, da, db, dw1, dw2, y, dx)]
        dw1, dw3, dw2, y, dx = pl.pallas_call(
            store_kernel,
            out_shape=(
                jax.ShapeDtypeStruct((d_model, d_ff), BF16),
                jax.ShapeDtypeStruct((d_model, d_ff), BF16),
                jax.ShapeDtypeStruct((d_ff, d_model), BF16),
                jax.ShapeDtypeStruct((n_tok, d_model), BF16),
                jax.ShapeDtypeStruct((n_tok, d_model), BF16),
            ),
            in_specs=[vmem] * 7,
            out_specs=(hbm,) * 5,
            scratch_shapes=[pltpu.VMEM((d_model, d_ff - HERE), BF16), up, dma((4,)), dma(((2 * d_ff - HERE) // PIECE,))],
            compiler_params=pltpu.CompilerParams(vmem_limit_bytes=16 * 2**20),
            name="store",
        )(*held)
        return y[None], dx[None], dw1[None, None], dw3[None, None], dw2[None, None]

    return jax.shard_map(
        device_fn,
        mesh=mesh,
        in_specs=(tok_spec, tok_spec, tok_spec, w_spec, w_spec, w_spec, tok_spec),
        out_specs=(tok_spec, tok_spec, w_spec, w_spec, w_spec),
        check_vma=False,
    )
```

```python
import functools

import jax
import jax.numpy as jnp
from jax import lax
from jax.experimental import pallas as pl
from jax.experimental.pallas import tpu as pltpu
from jax.sharding import PartitionSpec as P

MESH = pl.DeviceIdType.MESH
BF16 = jnp.bfloat16
F32 = jnp.float32
COL = 256
PIECE = 512
TILE = 256
CHUNKS = ((0, 4), (4, 8))
HERE = 1536
WIDE = 768
NT = (((1,), (1,)), ((), ()))
TN = (((0,), (0,)), ((), ()))
PEERS = ((0, 0, 0), (0, 0, 1), (1, 1, 0), (1, 1, 1), (0, 1, 0), (0, 1, 1), (1, 0, 0), (1, 0, 1))


def dot(lhs, rhs, dims=(((1,), (0,)), ((), ()))):
    return lax.dot_general(lhs, rhs, dims, preferred_element_type=F32)


def peer(me, place):
    y, x, core = PEERS[place]
    flip_y = lax.rem(me // 4 + y, 2)
    flip_x = lax.rem(lax.rem(me // 2, 2) + x, 2)
    return flip_y * 4 + flip_x * 2 + lax.rem(lax.rem(me, 2) + core, 2)


def slot_matrix(ids_row, n_exp, cap):
    n_tok = ids_row.shape[1]
    held = lax.broadcasted_iota(jnp.int32, (n_exp, n_tok), 0) == ids_row
    earlier = lax.broadcasted_iota(jnp.int32, (n_tok, n_tok), 0) < lax.broadcasted_iota(jnp.int32, (n_tok, n_tok), 1)
    counts = dot(held.astype(BF16), earlier.astype(BF16))
    rank = jnp.sum(jnp.where(held, counts, 0.0), axis=0, keepdims=True)
    slot = ids_row * cap + rank.astype(jnp.int32)
    return (lax.broadcasted_iota(jnp.int32, (n_exp * cap, n_tok), 0) == slot).astype(BF16)


def gate_column(gate_row):
    n_tok = gate_row.shape[1]
    eye = lax.broadcasted_iota(jnp.int32, (n_tok, n_tok), 0) == lax.broadcasted_iota(jnp.int32, (n_tok, n_tok), 1)
    return jnp.sum(jnp.where(eye, gate_row, 0.0), axis=1, keepdims=True)


def exchange_kernel(
    n_group, cap,
    ids_hbm, gate_hbm, x_hbm, dy_hbm, w1_hbm, w3_hbm, w2_hbm,
    perm, gate_m, back, xt, da_ref, db_ref, dw1, dw2,
    w1, w3, w2, w1t, w3t, w2t, xr, qr, h_ref, xs, qs, dxs, os, ids_m, tok_v,
    w_sem, in_sem, meta_sem, xsend, xrecv, qsend, qrecv, dxsend, dxrecv, osend, yrecv, pair_sem,
):
    stage = lax.axis_index("stage")
    me = lax.axis_index("expert")
    n_rows = n_group * cap
    d_model, d_ff = w1.shape
    n_col = d_model // COL
    on_a = stage == 0
    on_b = stage == 1

    def block(index):
        return pl.ds(pl.multiple_of(index * cap, 16), cap)

    def place(k):
        return pl.ds(k * cap, cap)

    def send(src, dst, send_sem, recv_sem, to_stage, to):
        pltpu.make_async_remote_copy(
            src_ref=src, dst_ref=dst, send_sem=send_sem, recv_sem=recv_sem,
            device_id=(to_stage, to), device_id_type=MESH,
        ).start()

    def wait_bytes(ref, sem):
        pltpu.make_async_copy(ref, ref, sem).wait()

    barrier = pltpu.get_barrier_semaphore()
    for other in range(1, 2 * n_group):
        flat = lax.rem(stage * n_group + me + other, 2 * n_group)
        pl.semaphore_signal(
            barrier, inc=1, device_id=(flat // n_group, lax.rem(flat, n_group)), device_id_type=MESH
        )
    loads = [pltpu.make_async_copy(src, dst, w_sem.at[i]) for i, (src, dst) in enumerate(((w2_hbm, w2), (w1_hbm, w1), (w3_hbm, w3)))]

    ids_load = pltpu.make_async_copy(ids_hbm, ids_m, in_sem.at[0])
    gate_load = pltpu.make_async_copy(gate_hbm, gate_m, in_sem.at[1])
    x_load = pltpu.make_async_copy(x_hbm, tok_v, in_sem.at[2])
    dy_load = pltpu.make_async_copy(dy_hbm, tok_v, in_sem.at[2])

    @pl.when(on_b)
    def _():
        dy_load.start()
        for load in loads:
            load.start()

    @pl.when(on_a)
    def _():
        ids_load.start()
        gate_load.start()
        x_load.start()
        ids_load.wait()
        gate_load.wait()
        perm[...] = slot_matrix(ids_m[...], n_group, cap)
        x_load.wait()
        xs[...] = dot(perm[...], tok_v[...]).astype(BF16)

    pl.semaphore_wait(barrier, 2 * n_group - 1)

    @pl.when(on_a)
    def _():
        send(ids_m, ids_m, meta_sem.at[0], meta_sem.at[2], 1, me)
        send(gate_m, gate_m, meta_sem.at[1], meta_sem.at[3], 1, me)
        for r, (lo, hi) in enumerate(CHUNKS):
            for k in range(lo, hi):
                to = peer(me, k)
                send(xs.at[block(to)], xr.at[place(k)], xsend.at[r], xrecv.at[r], 1, to)
            wait_bytes(xs.at[pl.ds(0, (hi - lo) * cap)], xsend.at[r])
            if r == 0:
                pl.semaphore_signal(pair_sem, inc=1, device_id=(0, peer(me, 1)), device_id_type=MESH)
                pl.semaphore_wait(pair_sem, 1)

        @pl.loop(0, d_ff // WIDE)
        def _(j):
            cols = pl.ds(pl.multiple_of(j * WIDE, WIDE), WIDE)
            dw2[cols, :] = jnp.zeros((WIDE, d_model), BF16)

        @pl.loop(0, HERE // WIDE)
        def _(j):
            cols = pl.ds(pl.multiple_of(j * WIDE, WIDE), WIDE)
            dw1[:, cols] = jnp.zeros((d_model, WIDE), BF16)

        for c in range(n_col):
            wait_bytes(back.at[c], dxrecv.at[c])
        wait_bytes(ids_m, meta_sem.at[0])
        wait_bytes(gate_m, meta_sem.at[1])

    @pl.when(on_b)
    def _():
        eye = (
            lax.broadcasted_iota(jnp.int32, (TILE, TILE), 0) == lax.broadcasted_iota(jnp.int32, (TILE, TILE), 1)
        ).astype(BF16)
        loads[0].wait()

        @pl.loop(0, d_ff // WIDE)
        def _(j):
            for c in range(n_col):
                wide = pl.ds(pl.multiple_of(j * WIDE, WIDE), WIDE)
                cols = slice(c * COL, (c + 1) * COL)
                w2t[cols, wide] = dot(eye, w2[wide, cols], NT).astype(BF16)

        wait_bytes(ids_m, meta_sem.at[2])
        wait_bytes(gate_m, meta_sem.at[3])
        perm[...] = slot_matrix(ids_m[...], n_group, cap)
        gate_col = gate_column(gate_m[...])
        dy_load.wait()
        gated = (gate_col * tok_v[...].astype(F32)).astype(BF16)
        qs[...] = dot(perm[...], gated).astype(BF16)

        def send_q(r):
            for k in range(max(1, CHUNKS[r][0]), CHUNKS[r][1]):
                to = peer(me, k)
                send(qs.at[block(to)], qr.at[place(k)], qsend, qrecv.at[r], 1, to)

        send_q(0)
        for load, src, dst in ((loads[1], w1, w1t), (loads[2], w3, w3t)):
            load.wait()

            @pl.loop(0, d_ff // WIDE)
            def _(j):
                for i in range(WIDE // TILE):
                    tile = pl.ds(pl.multiple_of(j * WIDE + i * TILE, TILE), TILE)
                    dst[tile, :] = dot(eye, src[:, tile], NT).astype(BF16)

        send_q(1)
        qr[place(0), :] = qs[block(me), :]
        for r, (lo, hi) in enumerate(CHUNKS):
            first = max(1, lo)
            wait_bytes(qr.at[pl.ds(first * cap, (hi - first) * cap)], qrecv.at[r])
            rows = slice(lo * cap, hi * cap)
            wait_bytes(xr.at[pl.ds(lo * cap, (hi - lo) * cap)], xrecv.at[r])
            for j in range(d_ff // TILE):
                cols = slice(j * TILE, (j + 1) * TILE)
                dh = dot(qr[rows, :], w2t[:, cols])
                a = dot(xr[rows, :], w1[:, cols])
                b = dot(xr[rows, :], w3[:, cols])
                sig = jax.nn.sigmoid(a)
                act = a * sig
                h_ref[rows, cols] = (act * b).astype(BF16)
                da_ref[rows, cols] = (dh * b * sig * (1.0 + a * (1.0 - sig))).astype(BF16)
                db_ref[rows, cols] = (dh * act).astype(BF16)

            def dx_piece(c):
                cols = pl.ds(pl.multiple_of(c * COL, COL), COL)
                dxs[c, rows, :] = (dot(da_ref[rows, :], w1t[:, cols]) + dot(db_ref[rows, :], w3t[:, cols])).astype(BF16)
                for k in range(lo, hi):
                    send(dxs.at[c, place(k)], back.at[c, block(me)], dxsend, dxrecv.at[c], 0, peer(me, k))

            pl.loop(0, n_col)(dx_piece)

            @pl.loop(0, n_col)
            def _(c):
                cols = pl.ds(pl.multiple_of(c * COL, COL), COL)
                os[c, rows, :] = dot(h_ref[rows, :], w2[:, cols]).astype(BF16)

            for k in range(lo, hi):
                if k > 0:
                    for c in range(n_col):
                        send(os.at[c, place(k)], back.at[c, block(me)], osend, yrecv, 1, peer(me, k))
            if r == 0:
                for c in range(n_col):
                    back[c, block(me), :] = os[c, place(0), :]

        @pl.loop(0, d_ff // WIDE)
        def _(j):
            cols = pl.ds(pl.multiple_of(j * WIDE, WIDE), WIDE)
            dw2[cols, :] = dot(h_ref[:, cols], qr[...], TN).astype(BF16)
        xt[...] = xr[...].T

        @pl.loop(0, HERE // WIDE)
        def _(j):
            cols = pl.ds(pl.multiple_of(j * WIDE, WIDE), WIDE)
            dw1[:, cols] = dot(xt[...], da_ref[:, cols]).astype(BF16)

        others = pl.ds(0, n_rows - cap)
        wait_bytes(back.at[:, others], yrecv)
        wait_bytes(qs.at[others], qsend)
        wait_bytes(dxs, dxsend)
        wait_bytes(os.at[:, others], osend)


def store_kernel(
    perm, gate, back, xt, da_ref, db_ref, dw1_in, dw2_in,
    dw1, dw3, dw2, y_out, dx_out, dw1_v, dw3_v, tok_v, zero_v, sem, piece_sem,
):
    stage = lax.axis_index("stage")
    d_ff = db_ref.shape[1]
    pairs = ((dw2_in, dw2), (dw1_in, dw1.at[:, pl.ds(0, HERE)]))
    copies = [pltpu.make_async_copy(src, dst, sem.at[i]) for i, (src, dst) in enumerate(pairs)]
    for copy in copies:
        copy.start()

    zero_v[...] = jnp.zeros_like(zero_v)

    def put_tokens(held, empty):
        tok_copies = [pltpu.make_async_copy(tok_v, held, sem.at[2]), pltpu.make_async_copy(zero_v, empty, sem.at[3])]
        for copy in tok_copies:
            copy.start()
        for copy in tok_copies:
            copy.wait()

    @pl.when(stage == 0)
    def _():
        places = [dw1.at[:, pl.ds(HERE, d_ff - HERE)], dw3.at[:, pl.ds(0, HERE)], dw3.at[:, pl.ds(HERE, d_ff - HERE)]]
        zeros = [pltpu.make_async_copy(dw1_in.at[:, pl.ds(0, dst.shape[1])], dst, piece_sem.at[i]) for i, dst in enumerate(places)]
        for copy in zeros:
            copy.start()
        for c in range(back.shape[0]):
            tok_v[:, c * COL:(c + 1) * COL] = dot(perm[...], back[c], TN).astype(BF16)
        put_tokens(dx_out, y_out)
        for copy in zeros:
            copy.wait()

    @pl.when(stage == 1)
    def _():
        gate_col = gate_column(gate[...])
        for c in range(back.shape[0]):
            tok_v[:, c * COL:(c + 1) * COL] = (gate_col * dot(perm[...], back[c], TN)).astype(BF16)
        pieces = []
        for grad, held, out, skip in ((da_ref, dw1_v, dw1, HERE), (db_ref, dw3_v, dw3, 0)):
            for j in range((d_ff - skip) // PIECE):
                here = pl.ds(j * PIECE, PIECE)
                there = pl.ds(skip + j * PIECE, PIECE)
                held[:, here] = dot(xt[...], grad[:, there]).astype(BF16)
                pieces.append(pltpu.make_async_copy(held.at[:, here], out.at[:, there], piece_sem.at[len(pieces)]))
                pieces[-1].start()
        put_tokens(y_out, dx_out)
        for piece in pieces:
            piece.wait()

    for copy in copies:
        copy.wait()


def solution(mesh):
    n_group = mesh.shape["expert"]
    tok_spec = P("stage", "expert", None)
    w_spec = P("stage", "expert", None, None)

    def device_fn(tokens_in, expert_ids, gate_wts, w_gate, w_up, w_down, grad_out):
        n_tok, d_model = tokens_in.shape[1:]
        d_ff = w_gate.shape[3]
        cap = 3 * n_tok // (2 * n_group)
        n_rows = n_group * cap
        vmem = pl.BlockSpec(memory_space=pltpu.VMEM)
        hbm = pl.BlockSpec(memory_space=pl.ANY)
        blocks = pltpu.VMEM((n_rows, d_model), BF16)
        pieces = pltpu.VMEM((d_model // COL, n_rows, COL), BF16)
        hidden = pltpu.VMEM((n_rows, d_ff), BF16)
        up = pltpu.VMEM((d_model, d_ff), BF16)
        down = pltpu.VMEM((d_ff, d_model), BF16)
        tok = pltpu.VMEM((n_tok, d_model), BF16)
        dma = pltpu.SemaphoreType.DMA
        perm, gate, back, xt, da, db, dw1, dw2 = pl.pallas_call(
            functools.partial(exchange_kernel, n_group, cap),
            out_shape=(
                pltpu.VMEM((n_rows, n_tok), BF16), pltpu.VMEM((1, n_tok), F32), pieces,
                pltpu.VMEM((d_model, n_rows), BF16), hidden, hidden, pltpu.VMEM((d_model, HERE), BF16), down,
            ),
            in_specs=[hbm] * 7,
            out_specs=(vmem,) * 8,
            scratch_shapes=[
                up, up, down, down, down, up, blocks, blocks, hidden,
                blocks, blocks, pieces, pieces,
                pltpu.VMEM((1, n_tok), jnp.int32),
                tok,
                dma((3,)),
                dma((3,)),
                dma((4,)),
                dma((len(CHUNKS),)),
                dma((len(CHUNKS),)),
                dma(()),
                dma((len(CHUNKS),)),
                dma(()),
                dma((d_model // COL,)),
                dma(()),
                dma(()),
                pltpu.SemaphoreType.REGULAR,
            ],
            compiler_params=pltpu.CompilerParams(
                collective_id=0, has_side_effects=True, vmem_limit_bytes=48 * 2**20
            ),
            name="exchange",
        )(*(pltpu.with_memory_space_constraint(v, pltpu.HBM) for v in (
            expert_ids.reshape(1, n_tok), gate_wts.reshape(1, n_tok), tokens_in[0], grad_out[0],
            w_gate[0, 0], w_up[0, 0], w_down[0, 0],
        )))
        held = [pltpu.with_memory_space_constraint(v, pltpu.VMEM) for v in (perm, gate, back, xt, da, db, dw1, dw2)]
        dw1, dw3, dw2, y, dx = pl.pallas_call(
            store_kernel,
            out_shape=(
                jax.ShapeDtypeStruct((d_model, d_ff), BF16),
                jax.ShapeDtypeStruct((d_model, d_ff), BF16),
                jax.ShapeDtypeStruct((d_ff, d_model), BF16),
                jax.ShapeDtypeStruct((n_tok, d_model), BF16),
                jax.ShapeDtypeStruct((n_tok, d_model), BF16),
            ),
            in_specs=[vmem] * 8,
            out_specs=(hbm,) * 5,
            scratch_shapes=[pltpu.VMEM((d_model, d_ff - HERE), BF16), up, tok, tok, dma((4,)), dma(((2 * d_ff - HERE) // PIECE,))],
            compiler_params=pltpu.CompilerParams(vmem_limit_bytes=16 * 2**20),
            name="store",
        )(*held)
        return y[None], dx[None], dw1[None, None], dw3[None, None], dw2[None, None]

    return jax.shard_map(
        device_fn,
        mesh=mesh,
        in_specs=(tok_spec, tok_spec, tok_spec, w_spec, w_spec, w_spec, tok_spec),
        out_specs=(tok_spec, tok_spec, w_spec, w_spec, w_spec),
        check_vma=False,
    )
```

```python
import functools

import jax
import jax.numpy as jnp
from jax import lax
from jax.experimental import pallas as pl
from jax.experimental.pallas import tpu as pltpu
from jax.sharding import PartitionSpec as P

MESH = pl.DeviceIdType.MESH
BF16 = jnp.bfloat16
F32 = jnp.float32
COL = 256
PIECE = 512
TILE = 256
CHUNKS = ((0, 4), (4, 8))
HERE = 1536
WIDE = 1536
NT = (((1,), (1,)), ((), ()))
TN = (((0,), (0,)), ((), ()))
PEERS = ((0, 0, 0), (0, 0, 1), (1, 1, 0), (1, 1, 1), (0, 1, 0), (0, 1, 1), (1, 0, 0), (1, 0, 1))


def dot(lhs, rhs, dims=(((1,), (0,)), ((), ()))):
    return lax.dot_general(lhs, rhs, dims, preferred_element_type=F32)


def peer(me, place):
    y, x, core = PEERS[place]
    flip_y = lax.rem(me // 4 + y, 2)
    flip_x = lax.rem(lax.rem(me // 2, 2) + x, 2)
    return flip_y * 4 + flip_x * 2 + lax.rem(lax.rem(me, 2) + core, 2)


def slot_matrix(ids_row, n_exp, cap):
    n_tok = ids_row.shape[1]
    held = lax.broadcasted_iota(jnp.int32, (n_exp, n_tok), 0) == ids_row
    earlier = lax.broadcasted_iota(jnp.int32, (n_tok, n_tok), 0) < lax.broadcasted_iota(jnp.int32, (n_tok, n_tok), 1)
    counts = dot(held.astype(BF16), earlier.astype(BF16))
    rank = jnp.sum(jnp.where(held, counts, 0.0), axis=0, keepdims=True)
    slot = ids_row * cap + rank.astype(jnp.int32)
    return (lax.broadcasted_iota(jnp.int32, (n_exp * cap, n_tok), 0) == slot).astype(BF16)


def gate_column(gate_row):
    n_tok = gate_row.shape[1]
    eye = lax.broadcasted_iota(jnp.int32, (n_tok, n_tok), 0) == lax.broadcasted_iota(jnp.int32, (n_tok, n_tok), 1)
    return jnp.sum(jnp.where(eye, gate_row, 0.0), axis=1, keepdims=True)


def exchange_kernel(
    n_group, cap,
    ids_hbm, gate_hbm, x_hbm, dy_hbm, w1_hbm, w3_hbm, w2_hbm,
    perm, gate_m, back, xt, da_ref, db_ref, dw1, dw2,
    w1, w3, w2, w1t, w3t, w2t, xr, qr, h_ref, xs, qs, dxs, os, ids_m, tok_v,
    w_sem, in_sem, meta_sem, xsend, xrecv, qsend, qrecv, dxsend, dxrecv, osend, yrecv, pair_sem,
):
    stage = lax.axis_index("stage")
    me = lax.axis_index("expert")
    n_rows = n_group * cap
    d_model, d_ff = w1.shape
    n_col = d_model // COL
    on_a = stage == 0
    on_b = stage == 1

    def block(index):
        return pl.ds(pl.multiple_of(index * cap, 16), cap)

    def place(k):
        return pl.ds(k * cap, cap)

    def send(src, dst, send_sem, recv_sem, to_stage, to):
        pltpu.make_async_remote_copy(
            src_ref=src, dst_ref=dst, send_sem=send_sem, recv_sem=recv_sem,
            device_id=(to_stage, to), device_id_type=MESH,
        ).start()

    def wait_bytes(ref, sem):
        pltpu.make_async_copy(ref, ref, sem).wait()

    barrier = pltpu.get_barrier_semaphore()
    for other in range(1, 2 * n_group):
        flat = lax.rem(stage * n_group + me + other, 2 * n_group)
        pl.semaphore_signal(
            barrier, inc=1, device_id=(flat // n_group, lax.rem(flat, n_group)), device_id_type=MESH
        )
    loads = [pltpu.make_async_copy(src, dst, w_sem.at[i]) for i, (src, dst) in enumerate(((w2_hbm, w2), (w1_hbm, w1), (w3_hbm, w3)))]

    ids_load = pltpu.make_async_copy(ids_hbm, ids_m, in_sem.at[0])
    gate_load = pltpu.make_async_copy(gate_hbm, gate_m, in_sem.at[1])
    x_load = pltpu.make_async_copy(x_hbm, tok_v, in_sem.at[2])
    dy_load = pltpu.make_async_copy(dy_hbm, tok_v, in_sem.at[2])

    @pl.when(on_b)
    def _():
        dy_load.start()
        for load in loads:
            load.start()

    @pl.when(on_a)
    def _():
        ids_load.start()
        gate_load.start()
        x_load.start()
        ids_load.wait()
        gate_load.wait()
        perm[...] = slot_matrix(ids_m[...], n_group, cap)
        x_load.wait()
        xs[...] = dot(perm[...], tok_v[...]).astype(BF16)

    pl.semaphore_wait(barrier, 2 * n_group - 1)

    @pl.when(on_a)
    def _():
        send(ids_m, ids_m, meta_sem.at[0], meta_sem.at[2], 1, me)
        send(gate_m, gate_m, meta_sem.at[1], meta_sem.at[3], 1, me)
        for r, (lo, hi) in enumerate(CHUNKS):
            for k in range(lo, hi):
                to = peer(me, k)
                send(xs.at[block(to)], xr.at[place(k)], xsend.at[r], xrecv.at[r], 1, to)
            wait_bytes(xs.at[pl.ds(0, (hi - lo) * cap)], xsend.at[r])
            if r == 0:
                pl.semaphore_signal(pair_sem, inc=1, device_id=(0, peer(me, 1)), device_id_type=MESH)
                pl.semaphore_wait(pair_sem, 1)

        @pl.loop(0, d_ff // WIDE)
        def _(j):
            cols = pl.ds(pl.multiple_of(j * WIDE, WIDE), WIDE)
            dw2[cols, :] = jnp.zeros((WIDE, d_model), BF16)

        @pl.loop(0, HERE // WIDE)
        def _(j):
            cols = pl.ds(pl.multiple_of(j * WIDE, WIDE), WIDE)
            dw1[:, cols] = jnp.zeros((d_model, WIDE), BF16)

        for c in range(n_col):
            wait_bytes(back.at[c], dxrecv.at[c])
        wait_bytes(ids_m, meta_sem.at[0])
        wait_bytes(gate_m, meta_sem.at[1])

    @pl.when(on_b)
    def _():
        eye = (
            lax.broadcasted_iota(jnp.int32, (TILE, TILE), 0) == lax.broadcasted_iota(jnp.int32, (TILE, TILE), 1)
        ).astype(BF16)
        loads[0].wait()

        @pl.loop(0, d_ff // WIDE)
        def _(j):
            for c in range(n_col):
                wide = pl.ds(pl.multiple_of(j * WIDE, WIDE), WIDE)
                cols = slice(c * COL, (c + 1) * COL)
                w2t[cols, wide] = dot(eye, w2[wide, cols], NT).astype(BF16)

        wait_bytes(ids_m, meta_sem.at[2])
        wait_bytes(gate_m, meta_sem.at[3])
        perm[...] = slot_matrix(ids_m[...], n_group, cap)
        gate_col = gate_column(gate_m[...])
        dy_load.wait()
        gated = (gate_col * tok_v[...].astype(F32)).astype(BF16)
        qs[...] = dot(perm[...], gated).astype(BF16)

        def send_q(r):
            for k in range(max(1, CHUNKS[r][0]), CHUNKS[r][1]):
                to = peer(me, k)
                send(qs.at[block(to)], qr.at[place(k)], qsend, qrecv.at[r], 1, to)

        send_q(0)
        for load, src, dst in ((loads[1], w1, w1t), (loads[2], w3, w3t)):
            load.wait()

            @pl.loop(0, d_ff // WIDE)
            def _(j):
                for i in range(WIDE // TILE):
                    tile = pl.ds(pl.multiple_of(j * WIDE + i * TILE, TILE), TILE)
                    dst[tile, :] = dot(eye, src[:, tile], NT).astype(BF16)

        send_q(1)
        qr[place(0), :] = qs[block(me), :]
        for r, (lo, hi) in enumerate(CHUNKS):
            first = max(1, lo)
            wait_bytes(qr.at[pl.ds(first * cap, (hi - first) * cap)], qrecv.at[r])
            rows = slice(lo * cap, hi * cap)
            wait_bytes(xr.at[pl.ds(lo * cap, (hi - lo) * cap)], xrecv.at[r])
            for j in range(d_ff // TILE):
                cols = slice(j * TILE, (j + 1) * TILE)
                dh = dot(qr[rows, :], w2t[:, cols])
                a = dot(xr[rows, :], w1[:, cols])
                b = dot(xr[rows, :], w3[:, cols])
                sig = jax.nn.sigmoid(a)
                act = a * sig
                h_ref[rows, cols] = (act * b).astype(BF16)
                da_ref[rows, cols] = (dh * b * (sig + act * (1.0 - sig))).astype(BF16)
                db_ref[rows, cols] = (dh * act).astype(BF16)

            def dx_piece(c):
                cols = pl.ds(pl.multiple_of(c * COL, COL), COL)
                dxs[c, rows, :] = (dot(da_ref[rows, :], w1t[:, cols]) + dot(db_ref[rows, :], w3t[:, cols])).astype(BF16)
                for k in range(lo, hi):
                    send(dxs.at[c, place(k)], back.at[c, block(me)], dxsend, dxrecv.at[c], 0, peer(me, k))

            pl.loop(0, n_col)(dx_piece)

            @pl.loop(0, n_col)
            def _(c):
                cols = pl.ds(pl.multiple_of(c * COL, COL), COL)
                os[c, rows, :] = dot(h_ref[rows, :], w2[:, cols]).astype(BF16)

            for k in range(lo, hi):
                if k > 0:
                    for c in range(n_col):
                        send(os.at[c, place(k)], back.at[c, block(me)], osend, yrecv, 1, peer(me, k))
            if r == 0:
                for c in range(n_col):
                    back[c, block(me), :] = os[c, place(0), :]

        @pl.loop(0, d_ff // WIDE)
        def _(j):
            cols = pl.ds(pl.multiple_of(j * WIDE, WIDE), WIDE)
            dw2[cols, :] = dot(h_ref[:, cols], qr[...], TN).astype(BF16)
        xt[...] = xr[...].T

        @pl.loop(0, HERE // WIDE)
        def _(j):
            cols = pl.ds(pl.multiple_of(j * WIDE, WIDE), WIDE)
            dw1[:, cols] = dot(xt[...], da_ref[:, cols]).astype(BF16)

        others = pl.ds(0, n_rows - cap)
        wait_bytes(back.at[:, others], yrecv)
        wait_bytes(qs.at[others], qsend)
        wait_bytes(dxs, dxsend)
        wait_bytes(os.at[:, others], osend)


def store_kernel(
    perm, gate, back, xt, da_ref, db_ref, dw1_in, dw2_in,
    dw1, dw3, dw2, y_out, dx_out, dw1_v, dw3_v, tok_v, zero_v, sem, piece_sem,
):
    stage = lax.axis_index("stage")
    d_ff = db_ref.shape[1]
    pairs = ((dw2_in, dw2), (dw1_in, dw1.at[:, pl.ds(0, HERE)]))
    copies = [pltpu.make_async_copy(src, dst, sem.at[i]) for i, (src, dst) in enumerate(pairs)]
    for copy in copies:
        copy.start()

    zero_v[...] = jnp.zeros_like(zero_v)

    def put_tokens(held, empty):
        tok_copies = [pltpu.make_async_copy(tok_v, held, sem.at[2]), pltpu.make_async_copy(zero_v, empty, sem.at[3])]
        for copy in tok_copies:
            copy.start()
        for copy in tok_copies:
            copy.wait()

    @pl.when(stage == 0)
    def _():
        places = [dw1.at[:, pl.ds(HERE, d_ff - HERE)], dw3.at[:, pl.ds(0, HERE)], dw3.at[:, pl.ds(HERE, d_ff - HERE)]]
        zeros = [pltpu.make_async_copy(dw1_in.at[:, pl.ds(0, dst.shape[1])], dst, piece_sem.at[i]) for i, dst in enumerate(places)]
        for copy in zeros:
            copy.start()
        for c in range(back.shape[0]):
            tok_v[:, c * COL:(c + 1) * COL] = dot(perm[...], back[c], TN).astype(BF16)
        put_tokens(dx_out, y_out)
        for copy in zeros:
            copy.wait()

    @pl.when(stage == 1)
    def _():
        gate_col = gate_column(gate[...])
        for c in range(back.shape[0]):
            tok_v[:, c * COL:(c + 1) * COL] = (gate_col * dot(perm[...], back[c], TN)).astype(BF16)
        pieces = []
        for grad, held, out, skip in ((da_ref, dw1_v, dw1, HERE), (db_ref, dw3_v, dw3, 0)):
            for j in range((d_ff - skip) // PIECE):
                here = pl.ds(j * PIECE, PIECE)
                there = pl.ds(skip + j * PIECE, PIECE)
                held[:, here] = dot(xt[...], grad[:, there]).astype(BF16)
                pieces.append(pltpu.make_async_copy(held.at[:, here], out.at[:, there], piece_sem.at[len(pieces)]))
                pieces[-1].start()
        put_tokens(y_out, dx_out)
        for piece in pieces:
            piece.wait()

    for copy in copies:
        copy.wait()


def solution(mesh):
    n_group = mesh.shape["expert"]
    tok_spec = P("stage", "expert", None)
    w_spec = P("stage", "expert", None, None)

    def device_fn(tokens_in, expert_ids, gate_wts, w_gate, w_up, w_down, grad_out):
        n_tok, d_model = tokens_in.shape[1:]
        d_ff = w_gate.shape[3]
        cap = 3 * n_tok // (2 * n_group)
        n_rows = n_group * cap
        vmem = pl.BlockSpec(memory_space=pltpu.VMEM)
        hbm = pl.BlockSpec(memory_space=pl.ANY)
        blocks = pltpu.VMEM((n_rows, d_model), BF16)
        pieces = pltpu.VMEM((d_model // COL, n_rows, COL), BF16)
        hidden = pltpu.VMEM((n_rows, d_ff), BF16)
        up = pltpu.VMEM((d_model, d_ff), BF16)
        down = pltpu.VMEM((d_ff, d_model), BF16)
        tok = pltpu.VMEM((n_tok, d_model), BF16)
        dma = pltpu.SemaphoreType.DMA
        perm, gate, back, xt, da, db, dw1, dw2 = pl.pallas_call(
            functools.partial(exchange_kernel, n_group, cap),
            out_shape=(
                pltpu.VMEM((n_rows, n_tok), BF16), pltpu.VMEM((1, n_tok), F32), pieces,
                pltpu.VMEM((d_model, n_rows), BF16), hidden, hidden, pltpu.VMEM((d_model, HERE), BF16), down,
            ),
            in_specs=[hbm] * 7,
            out_specs=(vmem,) * 8,
            scratch_shapes=[
                up, up, down, down, down, up, blocks, blocks, hidden,
                blocks, blocks, pieces, pieces,
                pltpu.VMEM((1, n_tok), jnp.int32),
                tok,
                dma((3,)),
                dma((3,)),
                dma((4,)),
                dma((len(CHUNKS),)),
                dma((len(CHUNKS),)),
                dma(()),
                dma((len(CHUNKS),)),
                dma(()),
                dma((d_model // COL,)),
                dma(()),
                dma(()),
                pltpu.SemaphoreType.REGULAR,
            ],
            compiler_params=pltpu.CompilerParams(
                collective_id=0, has_side_effects=True, vmem_limit_bytes=48 * 2**20
            ),
            name="exchange",
        )(*(pltpu.with_memory_space_constraint(v, pltpu.HBM) for v in (
            expert_ids.reshape(1, n_tok), gate_wts.reshape(1, n_tok), tokens_in[0], grad_out[0],
            w_gate[0, 0], w_up[0, 0], w_down[0, 0],
        )))
        held = [pltpu.with_memory_space_constraint(v, pltpu.VMEM) for v in (perm, gate, back, xt, da, db, dw1, dw2)]
        dw1, dw3, dw2, y, dx = pl.pallas_call(
            store_kernel,
            out_shape=(
                jax.ShapeDtypeStruct((d_model, d_ff), BF16),
                jax.ShapeDtypeStruct((d_model, d_ff), BF16),
                jax.ShapeDtypeStruct((d_ff, d_model), BF16),
                jax.ShapeDtypeStruct((n_tok, d_model), BF16),
                jax.ShapeDtypeStruct((n_tok, d_model), BF16),
            ),
            in_specs=[vmem] * 8,
            out_specs=(hbm,) * 5,
            scratch_shapes=[pltpu.VMEM((d_model, d_ff - HERE), BF16), up, tok, tok, dma((4,)), dma(((2 * d_ff - HERE) // PIECE,))],
            compiler_params=pltpu.CompilerParams(vmem_limit_bytes=16 * 2**20),
            name="store",
        )(*held)
        return y[None], dx[None], dw1[None, None], dw3[None, None], dw2[None, None]

    return jax.shard_map(
        device_fn,
        mesh=mesh,
        in_specs=(tok_spec, tok_spec, tok_spec, w_spec, w_spec, w_spec, tok_spec),
        out_specs=(tok_spec, tok_spec, w_spec, w_spec, w_spec),
        check_vma=False,
    )
```

```python
import functools

import jax
import jax.numpy as jnp
from jax import lax
from jax.experimental import pallas as pl
from jax.experimental.pallas import tpu as pltpu
from jax.sharding import PartitionSpec as P

MESH = pl.DeviceIdType.MESH
BF16 = jnp.bfloat16
F32 = jnp.float32
COL = 256
PIECE = 512
TILE = 256
CHUNKS = ((0, 4), (4, 8))
HERE = 1536
WIDE = 1536
NT = (((1,), (1,)), ((), ()))
TN = (((0,), (0,)), ((), ()))
PEERS = ((0, 0, 0), (0, 0, 1), (1, 1, 0), (1, 1, 1), (0, 1, 0), (0, 1, 1), (1, 0, 0), (1, 0, 1))


def dot(lhs, rhs, dims=(((1,), (0,)), ((), ()))):
    return lax.dot_general(lhs, rhs, dims, preferred_element_type=F32)


def peer(me, place):
    y, x, core = PEERS[place]
    flip_y = lax.rem(me // 4 + y, 2)
    flip_x = lax.rem(lax.rem(me // 2, 2) + x, 2)
    return flip_y * 4 + flip_x * 2 + lax.rem(lax.rem(me, 2) + core, 2)


def slot_matrix(ids_row, n_exp, cap):
    n_tok = ids_row.shape[1]
    held = lax.broadcasted_iota(jnp.int32, (n_exp, n_tok), 0) == ids_row
    earlier = lax.broadcasted_iota(jnp.int32, (n_tok, n_tok), 0) < lax.broadcasted_iota(jnp.int32, (n_tok, n_tok), 1)
    counts = dot(held.astype(BF16), earlier.astype(BF16))
    rank = jnp.sum(jnp.where(held, counts, 0.0), axis=0, keepdims=True)
    slot = ids_row * cap + rank.astype(jnp.int32)
    return (lax.broadcasted_iota(jnp.int32, (n_exp * cap, n_tok), 0) == slot).astype(BF16)


def gate_column(gate_row):
    n_tok = gate_row.shape[1]
    eye = lax.broadcasted_iota(jnp.int32, (n_tok, n_tok), 0) == lax.broadcasted_iota(jnp.int32, (n_tok, n_tok), 1)
    return jnp.sum(jnp.where(eye, gate_row, 0.0), axis=1, keepdims=True)


def exchange_kernel(
    n_group, cap,
    ids_hbm, gate_hbm, x_hbm, dy_hbm, w1_hbm, w3_hbm, w2_hbm,
    perm, gate_m, back, xt, da_ref, db_ref, dw1, dw2,
    w1, w3, w2, w1t, w3t, w2t, xr, qr, h_ref, xs, qs, dxs, os, ids_m, tok_v,
    w_sem, in_sem, meta_sem, xsend, xrecv, qsend, qrecv, dxsend, dxrecv, osend, yrecv, pair_sem,
):
    stage = lax.axis_index("stage")
    me = lax.axis_index("expert")
    n_rows = n_group * cap
    d_model, d_ff = w1.shape
    n_col = d_model // COL
    on_a = stage == 0
    on_b = stage == 1

    def block(index):
        return pl.ds(pl.multiple_of(index * cap, 16), cap)

    def place(k):
        return pl.ds(k * cap, cap)

    def send(src, dst, send_sem, recv_sem, to_stage, to):
        pltpu.make_async_remote_copy(
            src_ref=src, dst_ref=dst, send_sem=send_sem, recv_sem=recv_sem,
            device_id=(to_stage, to), device_id_type=MESH,
        ).start()

    def wait_bytes(ref, sem):
        pltpu.make_async_copy(ref, ref, sem).wait()

    barrier = pltpu.get_barrier_semaphore()
    for other in range(1, 2 * n_group):
        flat = lax.rem(stage * n_group + me + other, 2 * n_group)
        pl.semaphore_signal(
            barrier, inc=1, device_id=(flat // n_group, lax.rem(flat, n_group)), device_id_type=MESH
        )
    loads = [pltpu.make_async_copy(src, dst, w_sem.at[i]) for i, (src, dst) in enumerate(((w2_hbm, w2), (w1_hbm, w1), (w3_hbm, w3)))]

    ids_load = pltpu.make_async_copy(ids_hbm, ids_m, in_sem.at[0])
    gate_load = pltpu.make_async_copy(gate_hbm, gate_m, in_sem.at[1])
    x_load = pltpu.make_async_copy(x_hbm, tok_v, in_sem.at[2])
    dy_load = pltpu.make_async_copy(dy_hbm, tok_v, in_sem.at[2])

    @pl.when(on_b)
    def _():
        dy_load.start()
        for load in loads:
            load.start()

    @pl.when(on_a)
    def _():
        ids_load.start()
        gate_load.start()
        x_load.start()
        ids_load.wait()
        gate_load.wait()
        perm[...] = slot_matrix(ids_m[...], n_group, cap)
        x_load.wait()
        xs[...] = dot(perm[...], tok_v[...]).astype(BF16)

    pl.semaphore_wait(barrier, 2 * n_group - 1)

    @pl.when(on_a)
    def _():
        send(ids_m, ids_m, meta_sem.at[0], meta_sem.at[2], 1, me)
        send(gate_m, gate_m, meta_sem.at[1], meta_sem.at[3], 1, me)
        for r, (lo, hi) in enumerate(CHUNKS):
            for k in range(lo, hi):
                to = peer(me, k)
                send(xs.at[block(to)], xr.at[place(k)], xsend.at[r], xrecv.at[r], 1, to)
            wait_bytes(xs.at[pl.ds(0, (hi - lo) * cap)], xsend.at[r])
            if r == 0:
                pl.semaphore_signal(pair_sem, inc=1, device_id=(0, peer(me, 1)), device_id_type=MESH)
                pl.semaphore_wait(pair_sem, 1)

        @pl.loop(0, d_ff // WIDE)
        def _(j):
            cols = pl.ds(pl.multiple_of(j * WIDE, WIDE), WIDE)
            dw2[cols, :] = jnp.zeros((WIDE, d_model), BF16)

        @pl.loop(0, HERE // WIDE)
        def _(j):
            cols = pl.ds(pl.multiple_of(j * WIDE, WIDE), WIDE)
            dw1[:, cols] = jnp.zeros((d_model, WIDE), BF16)

        for c in range(n_col):
            wait_bytes(back.at[c], dxrecv.at[c])
        wait_bytes(ids_m, meta_sem.at[0])
        wait_bytes(gate_m, meta_sem.at[1])

    @pl.when(on_b)
    def _():
        eye = (
            lax.broadcasted_iota(jnp.int32, (TILE, TILE), 0) == lax.broadcasted_iota(jnp.int32, (TILE, TILE), 1)
        ).astype(BF16)
        loads[0].wait()

        @pl.loop(0, d_ff // WIDE)
        def _(j):
            for c in range(n_col):
                wide = pl.ds(pl.multiple_of(j * WIDE, WIDE), WIDE)
                cols = slice(c * COL, (c + 1) * COL)
                w2t[cols, wide] = dot(eye, w2[wide, cols], NT).astype(BF16)

        wait_bytes(ids_m, meta_sem.at[2])
        wait_bytes(gate_m, meta_sem.at[3])
        perm[...] = slot_matrix(ids_m[...], n_group, cap)
        gate_col = gate_column(gate_m[...])
        dy_load.wait()
        gated = (gate_col * tok_v[...].astype(F32)).astype(BF16)
        qs[...] = dot(perm[...], gated).astype(BF16)

        def send_q(r):
            for k in range(max(1, CHUNKS[r][0]), CHUNKS[r][1]):
                to = peer(me, k)
                send(qs.at[block(to)], qr.at[place(k)], qsend, qrecv.at[r], 1, to)

        send_q(0)
        for load, src, dst in ((loads[1], w1, w1t), (loads[2], w3, w3t)):
            load.wait()

            @pl.loop(0, d_ff // WIDE)
            def _(j):
                for i in range(WIDE // TILE):
                    tile = pl.ds(pl.multiple_of(j * WIDE + i * TILE, TILE), TILE)
                    dst[tile, :] = dot(eye, src[:, tile], NT).astype(BF16)

        send_q(1)
        qr[place(0), :] = qs[block(me), :]
        for r, (lo, hi) in enumerate(CHUNKS):
            first = max(1, lo)
            wait_bytes(qr.at[pl.ds(first * cap, (hi - first) * cap)], qrecv.at[r])
            rows = slice(lo * cap, hi * cap)
            wait_bytes(xr.at[pl.ds(lo * cap, (hi - lo) * cap)], xrecv.at[r])
            for j in range(d_ff // TILE):
                cols = slice(j * TILE, (j + 1) * TILE)
                dh = dot(qr[rows, :], w2t[:, cols])
                a = dot(xr[rows, :], w1[:, cols])
                b = dot(xr[rows, :], w3[:, cols])
                sig = jax.nn.sigmoid(a)
                act = a * sig
                h_ref[rows, cols] = (act * b).astype(BF16)
                da_ref[rows, cols] = (dh * b * (sig + act * (1.0 - sig))).astype(BF16)
                db_ref[rows, cols] = (dh * act).astype(BF16)

            def dx_piece(c):
                cols = pl.ds(pl.multiple_of(c * COL, COL), COL)
                dxs[c, rows, :] = (dot(da_ref[rows, :], w1t[:, cols]) + dot(db_ref[rows, :], w3t[:, cols])).astype(BF16)
                for k in range(lo, hi):
                    send(dxs.at[c, place(k)], back.at[c, block(me)], dxsend, dxrecv.at[c], 0, peer(me, k))

            pl.loop(0, n_col)(dx_piece)

            @pl.loop(0, n_col)
            def _(c):
                cols = pl.ds(pl.multiple_of(c * COL, COL), COL)
                os[c, rows, :] = dot(h_ref[rows, :], w2[:, cols]).astype(BF16)
                for k in range(max(1, lo), hi):
                    send(os.at[c, place(k)], back.at[c, block(me)], osend, yrecv, 1, peer(me, k))

            if r == 0:
                for c in range(n_col):
                    back[c, block(me), :] = os[c, place(0), :]

        @pl.loop(0, d_ff // WIDE)
        def _(j):
            cols = pl.ds(pl.multiple_of(j * WIDE, WIDE), WIDE)
            dw2[cols, :] = dot(h_ref[:, cols], qr[...], TN).astype(BF16)
        xt[...] = xr[...].T

        @pl.loop(0, HERE // WIDE)
        def _(j):
            cols = pl.ds(pl.multiple_of(j * WIDE, WIDE), WIDE)
            dw1[:, cols] = dot(xt[...], da_ref[:, cols]).astype(BF16)

        others = pl.ds(0, n_rows - cap)
        wait_bytes(back.at[:, others], yrecv)
        wait_bytes(qs.at[others], qsend)
        wait_bytes(dxs, dxsend)
        wait_bytes(os.at[:, others], osend)


def store_kernel(
    perm, gate, back, xt, da_ref, db_ref, dw1_in, dw2_in,
    dw1, dw3, dw2, y_out, dx_out, dw1_v, dw3_v, tok_v, zero_v, sem, piece_sem,
):
    stage = lax.axis_index("stage")
    d_ff = db_ref.shape[1]
    pairs = ((dw2_in, dw2), (dw1_in, dw1.at[:, pl.ds(0, HERE)]))
    copies = [pltpu.make_async_copy(src, dst, sem.at[i]) for i, (src, dst) in enumerate(pairs)]
    for copy in copies:
        copy.start()

    zero_v[...] = jnp.zeros_like(zero_v)

    def put_tokens(held, empty):
        tok_copies = [pltpu.make_async_copy(tok_v, held, sem.at[2]), pltpu.make_async_copy(zero_v, empty, sem.at[3])]
        for copy in tok_copies:
            copy.start()
        for copy in tok_copies:
            copy.wait()

    @pl.when(stage == 0)
    def _():
        places = [dw1.at[:, pl.ds(HERE, d_ff - HERE)], dw3.at[:, pl.ds(0, HERE)], dw3.at[:, pl.ds(HERE, d_ff - HERE)]]
        zeros = [pltpu.make_async_copy(dw1_in.at[:, pl.ds(0, dst.shape[1])], dst, piece_sem.at[i]) for i, dst in enumerate(places)]
        for copy in zeros:
            copy.start()
        for c in range(back.shape[0]):
            tok_v[:, c * COL:(c + 1) * COL] = dot(perm[...], back[c], TN).astype(BF16)
        put_tokens(dx_out, y_out)
        for copy in zeros:
            copy.wait()

    @pl.when(stage == 1)
    def _():
        gate_col = gate_column(gate[...])
        for c in range(back.shape[0]):
            tok_v[:, c * COL:(c + 1) * COL] = (gate_col * dot(perm[...], back[c], TN)).astype(BF16)
        pieces = []
        for grad, held, out, skip in ((da_ref, dw1_v, dw1, HERE), (db_ref, dw3_v, dw3, 0)):
            for j in range((d_ff - skip) // PIECE):
                here = pl.ds(j * PIECE, PIECE)
                there = pl.ds(skip + j * PIECE, PIECE)
                held[:, here] = dot(xt[...], grad[:, there]).astype(BF16)
                pieces.append(pltpu.make_async_copy(held.at[:, here], out.at[:, there], piece_sem.at[len(pieces)]))
                pieces[-1].start()
        put_tokens(y_out, dx_out)
        for piece in pieces:
            piece.wait()

    for copy in copies:
        copy.wait()


def solution(mesh):
    n_group = mesh.shape["expert"]
    tok_spec = P("stage", "expert", None)
    w_spec = P("stage", "expert", None, None)

    def device_fn(tokens_in, expert_ids, gate_wts, w_gate, w_up, w_down, grad_out):
        n_tok, d_model = tokens_in.shape[1:]
        d_ff = w_gate.shape[3]
        cap = 3 * n_tok // (2 * n_group)
        n_rows = n_group * cap
        vmem = pl.BlockSpec(memory_space=pltpu.VMEM)
        hbm = pl.BlockSpec(memory_space=pl.ANY)
        blocks = pltpu.VMEM((n_rows, d_model), BF16)
        pieces = pltpu.VMEM((d_model // COL, n_rows, COL), BF16)
        hidden = pltpu.VMEM((n_rows, d_ff), BF16)
        up = pltpu.VMEM((d_model, d_ff), BF16)
        down = pltpu.VMEM((d_ff, d_model), BF16)
        tok = pltpu.VMEM((n_tok, d_model), BF16)
        dma = pltpu.SemaphoreType.DMA
        perm, gate, back, xt, da, db, dw1, dw2 = pl.pallas_call(
            functools.partial(exchange_kernel, n_group, cap),
            out_shape=(
                pltpu.VMEM((n_rows, n_tok), BF16), pltpu.VMEM((1, n_tok), F32), pieces,
                pltpu.VMEM((d_model, n_rows), BF16), hidden, hidden, pltpu.VMEM((d_model, HERE), BF16), down,
            ),
            in_specs=[hbm] * 7,
            out_specs=(vmem,) * 8,
            scratch_shapes=[
                up, up, down, down, down, up, blocks, blocks, hidden,
                blocks, blocks, pieces, pieces,
                pltpu.VMEM((1, n_tok), jnp.int32),
                tok,
                dma((3,)),
                dma((3,)),
                dma((4,)),
                dma((len(CHUNKS),)),
                dma((len(CHUNKS),)),
                dma(()),
                dma((len(CHUNKS),)),
                dma(()),
                dma((d_model // COL,)),
                dma(()),
                dma(()),
                pltpu.SemaphoreType.REGULAR,
            ],
            compiler_params=pltpu.CompilerParams(
                collective_id=0, has_side_effects=True, vmem_limit_bytes=48 * 2**20
            ),
            name="exchange",
        )(*(pltpu.with_memory_space_constraint(v, pltpu.HBM) for v in (
            expert_ids.reshape(1, n_tok), gate_wts.reshape(1, n_tok), tokens_in[0], grad_out[0],
            w_gate[0, 0], w_up[0, 0], w_down[0, 0],
        )))
        held = [pltpu.with_memory_space_constraint(v, pltpu.VMEM) for v in (perm, gate, back, xt, da, db, dw1, dw2)]
        dw1, dw3, dw2, y, dx = pl.pallas_call(
            store_kernel,
            out_shape=(
                jax.ShapeDtypeStruct((d_model, d_ff), BF16),
                jax.ShapeDtypeStruct((d_model, d_ff), BF16),
                jax.ShapeDtypeStruct((d_ff, d_model), BF16),
                jax.ShapeDtypeStruct((n_tok, d_model), BF16),
                jax.ShapeDtypeStruct((n_tok, d_model), BF16),
            ),
            in_specs=[vmem] * 8,
            out_specs=(hbm,) * 5,
            scratch_shapes=[pltpu.VMEM((d_model, d_ff - HERE), BF16), up, tok, tok, dma((4,)), dma(((2 * d_ff - HERE) // PIECE,))],
            compiler_params=pltpu.CompilerParams(vmem_limit_bytes=16 * 2**20),
            name="store",
        )(*held)
        return y[None], dx[None], dw1[None, None], dw3[None, None], dw2[None, None]

    return jax.shard_map(
        device_fn,
        mesh=mesh,
        in_specs=(tok_spec, tok_spec, tok_spec, w_spec, w_spec, w_spec, tok_spec),
        out_specs=(tok_spec, tok_spec, w_spec, w_spec, w_spec),
        check_vma=False,
    )
```
